128 devices in a mesh: ens: 1, feat: 128 (over z, y, x, core).
Axes of the slice: x: 4, y: 4, z: 4, core: 2. Of those that a mesh axis runs over, the one named last changes fastest.
Arguments:
- particles: float32 [2, 256, 32768], P('ens', None, 'feat')
- target_mean: float32 [2, 32768], P('ens', 'feat')
- precision: float32 [32768], P(('ens', 'feat'))
- low_factor: bfloat16 [32768, 64], P(('ens', 'feat'))
Outputs:
- output: float32 [2, 256, 32768], P('ens', None, 'feat')
All inputs are finite; a program needn't handle non-finite values.
Results may differ from the reference program's by a relative error of at most 0.001.
Values are sent between devices in bfloat16 or wider.
A program may use at most 1 GiB of HBM per device.

```python
import jax
import jax.numpy as jnp
from jax import lax

PARTICLES = 256
FEATURES = 32768
LOW_RANK = 64
NUM_STEPS = 3


def setup_inputs(seed: int = 0, part: int = 0) -> dict:
    base_key = jax.random.fold_in(jax.random.key(seed), part)
    key_list = jax.random.split(base_key, 7)
    prec_scale = 2.0 / FEATURES
    factor_scale = prec_scale ** 0.5 / FEATURES ** 0.5
    low_raw = factor_scale * jax.random.normal(key_list[0], (FEATURES, LOW_RANK), jnp.float32)
    precision = prec_scale * jax.random.uniform(key_list[1], (FEATURES,), jnp.float32, 0.5, 1.5)
    target_mean = jax.random.normal(key_list[2], (2, FEATURES), jnp.float32)
    center = 0.7 * jax.random.normal(key_list[3], (2, FEATURES), jnp.float32)
    coef_vec = jax.random.normal(key_list[4], (2, LOW_RANK), jnp.float32)
    aligned = jnp.dot(coef_vec, low_raw.T) * (0.7 / (factor_scale * LOW_RANK ** 0.5))
    spread = jax.random.uniform(key_list[5], (2, PARTICLES, 1), jnp.float32, 0.5, 1.5)
    noise_mat = jax.random.normal(key_list[6], (2, PARTICLES, FEATURES), jnp.float32)
    particles = (target_mean + center + aligned)[:, None, :] + spread * noise_mat
    return {"particles": particles, "target_mean": target_mean, "precision": precision, "low_factor": low_raw.astype(jnp.bfloat16)}


def svgd_step(theta, target_mean, precision, low_factor):
    bandwidth = 2.0 * FEATURES
    step_size = 0.25 * FEATURES
    low_wide = low_factor.astype(jnp.float32)
    centered = theta - target_mean[:, None, :]
    project = jnp.einsum("end,dr->enr", centered.astype(jnp.bfloat16).astype(jnp.float32), low_wide)
    theta_wide = theta.astype(jnp.bfloat16).astype(jnp.float32)
    gram_mat = jnp.einsum("end,emd->enm", theta_wide, theta_wide)
    gram_diag = jnp.diagonal(gram_mat, axis1=1, axis2=2)
    sq_dist = jnp.maximum(gram_diag[:, :, None] + gram_diag[:, None, :] - 2.0 * gram_mat, 0.0)
    kernel = jnp.exp(-sq_dist / bandwidth)
    low_term = jnp.einsum("enr,dr->end", project.astype(jnp.bfloat16).astype(jnp.float32), low_wide)
    grad_log = -(centered * precision + low_term)
    mixed = (grad_log - (2.0 / bandwidth) * theta).astype(jnp.bfloat16).astype(jnp.float32)
    drive = jnp.einsum("enm,emd->end", kernel.astype(jnp.bfloat16).astype(jnp.float32), mixed)
    row_sum = jnp.sum(kernel, axis=2, keepdims=True)
    return theta + step_size * ((drive + (2.0 / bandwidth) * row_sum * theta) / PARTICLES)


def reference(particles, target_mean, precision, low_factor):
    def scan_body(theta, unused):
        return svgd_step(theta, target_mean, precision, low_factor), None
    final_theta, unused_out = lax.scan(scan_body, particles, None, length=NUM_STEPS)
    return final_theta
```

```python
import functools

import jax
import jax.numpy as jnp
from jax import lax
from jax.experimental import pallas as pl
from jax.experimental.pallas import tpu as pltpu
from jax.sharding import PartitionSpec as P

NUM_STEPS = 3
SIDE = 4
CHIPS = SIDE ** 3
HALF = 128
MESH = pl.DeviceIdType.MESH
NT = (((1,), (1,)), ((), ()))


def _hops(offset):
    return sum(min(d, SIDE - d) for d in offset)


OFFSETS = sorted(
    [(a, b, c) for a in range(SIDE) for b in range(SIDE) for c in range(SIDE) if (a, b, c) != (0, 0, 0)],
    key=lambda offset: -_hops(offset),
)


def _kernel(consts, part_ref, mean_ref, prec_ref, factor_ref, out_ref,
            theta, mean_x, prec_x, factor_x, rs_send, rs_recv, gather, u_lo, u_hi,
            load_sem, swap_send, swap_recv, rs_ssem, rs_rsem, ag_ssem, ag_rsem, out_sem, back_send, back_recv):
    two_over_h, inv_h, step_size, inv_part = consts
    feat = factor_ref.shape[0]
    rank = factor_ref.shape[1]
    f32, bf16 = jnp.float32, jnp.bfloat16
    ens = lax.axis_index("ens")
    me = lax.axis_index("feat")
    core = me % 2
    chip = me // 2
    px, py, pz = chip % SIDE, (chip // SIDE) % SIDE, chip // (SIDE * SIDE)
    partner = chip * 2 + (1 - core)

    def peer(offset):
        dz, dy, dx = offset
        tz, ty, tx = (pz + dz) % SIDE, (py + dy) % SIDE, (px + dx) % SIDE
        return (tz * SIDE + ty) * SIDE + tx

    barrier = pltpu.get_barrier_semaphore()
    for offset in OFFSETS:
        pl.semaphore_signal(barrier, inc=1, device_id=(ens, peer(offset) * 2 + core), device_id_type=MESH)
    pl.semaphore_signal(barrier, inc=1, device_id=(ens, partner), device_id_type=MESH)
    load = pltpu.make_async_copy(part_ref.at[core], theta.at[:, pl.ds(0, feat)], load_sem)
    load.start()
    pl.semaphore_wait(barrier, CHIPS)

    swaps = []
    for k, (src, dst) in enumerate((
        (part_ref.at[1 - core], theta.at[:, pl.ds(feat, feat)]),
        (mean_ref, mean_x), (prec_ref, prec_x), (factor_ref, factor_x),
    )):
        copy = pltpu.make_async_remote_copy(src, dst, swap_send.at[k], swap_recv.at[k], device_id=(ens, partner), device_id_type=MESH)
        copy.start()
        swaps.append(copy)
    load.wait()
    for copy in swaps:
        copy.wait_recv()

    row_id = lax.broadcasted_iota(jnp.int32, (HALF, HALF), 0)
    col_id = lax.broadcasted_iota(jnp.int32, (HALF, HALF), 1)
    eye, upper = row_id == col_id, row_id <= col_id

    for part, ref in enumerate((factor_ref, factor_x)):
        rows = pl.ds(part * feat, feat)
        zeros = jnp.zeros((feat, HALF - rank), bf16)
        u_lo[rows, :] = jnp.concatenate([ref[...], zeros], axis=1)
        u_hi[rows, :] = jnp.concatenate([zeros, ref[...]], axis=1)
    mean_row = jnp.concatenate([mean_ref[pl.ds(core, 1), :], mean_x[pl.ds(core, 1), :]], axis=1)
    prec_row = jnp.concatenate([prec_ref[...], prec_x[...]], axis=1)

    def partials():
        th = theta[...]
        tb = th.astype(bf16)
        xb = (th - mean_row).astype(bf16)
        top = lax.dot_general(tb[:HALF], tb, NT, preferred_element_type=f32)
        low = lax.dot_general(tb[HALF:], tb[HALF:], NT, preferred_element_type=f32)
        proj = (jnp.dot(xb[:HALF], u_lo[...], preferred_element_type=f32)
                + jnp.dot(xb[HALF:], u_hi[...], preferred_element_type=f32))
        tri = jnp.where(upper, top[:, :HALF], low)
        cross = top[:, HALF:]
        diag = jnp.sum(jnp.where(eye, low, 0.0), axis=0, keepdims=True)
        for o in range(CHIPS):
            block, r = (cross, 4 * o) if o < CHIPS // 2 else (tri, 4 * o - HALF)
            rs_send[o, 0:4, :] = block[r:r + 4]
            rs_send[o, 4:6, :] = proj[2 * o:2 * o + 2]
            rs_send[o, 6:7, :] = diag

    def all_reduce():
        for offset in OFFSETS:
            target = peer(offset)
            pltpu.make_async_remote_copy(
                rs_send.at[target], rs_recv.at[chip], rs_ssem, rs_rsem,
                device_id=(ens, target * 2 + core), device_id_type=MESH).start()
        rs_recv[chip] = rs_send[chip]
        others = pl.ds(0, CHIPS - 1)
        pltpu.make_async_copy(rs_recv.at[others], rs_recv.at[others], rs_rsem).wait()
        total = rs_recv[0]
        for o in range(1, CHIPS):
            total = total + rs_recv[o]
        gather[chip] = total[:6]
        for offset in OFFSETS:
            target = peer(offset)
            pltpu.make_async_remote_copy(
                gather.at[chip], gather.at[chip], ag_ssem, ag_rsem,
                device_id=(ens, target * 2 + core), device_id_type=MESH).start()
        pltpu.make_async_copy(gather.at[others], gather.at[others], ag_rsem).wait()
        pltpu.make_async_copy(rs_send.at[others], rs_send.at[others], rs_ssem).wait()
        pltpu.make_async_copy(gather.at[others], gather.at[others], ag_ssem).wait()
        return total[6:7]

    def update(diag):
        cross = jnp.concatenate([gather[o, 0:4, :] for o in range(CHIPS // 2)], axis=0)
        tri = jnp.concatenate([gather[o, 0:4, :] for o in range(CHIPS // 2, CHIPS)], axis=0)
        proj = jnp.concatenate([gather[o, 4:6, :] for o in range(CHIPS)], axis=0).astype(bf16)
        tri_t, cross_t = tri.T, cross.T
        g_aa = jnp.where(upper, tri, tri_t)
        g_cc = jnp.where(eye, diag, jnp.where(upper, tri_t, tri))
        row_a = jnp.sum(jnp.where(eye, tri, 0.0), axis=0, keepdims=True)
        col_a = jnp.sum(jnp.where(eye, tri, 0.0), axis=1, keepdims=True)
        col_c = jnp.sum(jnp.where(eye, diag, 0.0), axis=1, keepdims=True)
        top = jnp.concatenate([g_aa, cross], axis=1)
        bottom = jnp.concatenate([cross_t, g_cc], axis=1)
        row_all = jnp.concatenate([row_a, diag], axis=1)
        k_top = jnp.exp(-jnp.maximum(col_a + row_all - 2.0 * top, 0.0) * inv_h)
        k_bot = jnp.exp(-jnp.maximum(col_c + row_all - 2.0 * bottom, 0.0) * inv_h)
        kernel = jnp.concatenate([k_top, k_bot], axis=0)
        row_sum = jnp.sum(kernel, axis=1, keepdims=True)
        kernel_bf = kernel.astype(bf16)
        for part in range(2):
            cols = slice(part * feat, (part + 1) * feat)
            th = theta[:, cols]
            low = jnp.concatenate([
                lax.dot_general(proj, u_lo[cols, :], NT, preferred_element_type=f32),
                lax.dot_general(proj, u_hi[cols, :], NT, preferred_element_type=f32)], axis=0)
            grad = -((th - mean_row[:, cols]) * prec_row[:, cols] + low)
            mixed = (grad - two_over_h * th).astype(bf16)
            drive = jnp.dot(kernel_bf, mixed, preferred_element_type=f32)
            theta[:, cols] = th + step_size * ((drive + two_over_h * row_sum * th) * inv_part)

    partials()

    @pl.loop(0, NUM_STEPS - 1)
    def _(_):
        update(all_reduce())
        partials()

    update(all_reduce())

    back = pltpu.make_async_remote_copy(theta.at[:, pl.ds(feat, feat)], out_ref.at[core], back_send, back_recv, device_id=(ens, partner), device_id_type=MESH)
    back.start()
    keep = pltpu.make_async_copy(theta.at[:, pl.ds(0, feat)], out_ref.at[core], out_sem)
    keep.start()
    for copy in swaps:
        copy.wait_send()
    keep.wait()
    pltpu.make_async_remote_copy(theta.at[:, pl.ds(feat, feat)], out_ref.at[1 - core], back_send, back_recv, device_id=(ens, partner), device_id_type=MESH).wait()


def solution(mesh):
    feat_count = mesh.shape["feat"]
    data_spec = P("ens", None, "feat")
    mean_spec = P("ens", "feat")
    prec_spec = P(("ens", "feat"))
    factor_spec = P(("ens", "feat"), None)

    def local_steps(particles, target_mean, precision, low_factor):
        _, num_part, feat = particles.shape
        rank = low_factor.shape[1]
        total_feat = feat * feat_count
        bandwidth = 2.0 * total_feat
        consts = (2.0 / bandwidth, 1.0 / bandwidth, 0.25 * total_feat, 1.0 / num_part)
        vmem, hbm = pl.BlockSpec(memory_space=pltpu.VMEM), pl.BlockSpec(memory_space=pl.ANY)
        dma = pltpu.SemaphoreType.DMA
        return pl.pallas_call(
            functools.partial(_kernel, consts),
            name="svgd",
            out_shape=jax.ShapeDtypeStruct(particles.shape, jnp.float32),
            in_specs=[hbm, vmem, vmem, vmem],
            out_specs=hbm,
            scratch_shapes=[
                pltpu.VMEM((num_part, 2 * feat), jnp.float32),
                pltpu.VMEM((2, feat), jnp.float32),
                pltpu.VMEM((1, feat), jnp.float32),
                pltpu.VMEM((feat, rank), jnp.bfloat16),
                pltpu.VMEM((CHIPS, 7, HALF), jnp.float32),
                pltpu.VMEM((CHIPS, 7, HALF), jnp.float32),
                pltpu.VMEM((CHIPS, 6, HALF), jnp.float32),
                pltpu.VMEM((2 * feat, HALF), jnp.bfloat16),
                pltpu.VMEM((2 * feat, HALF), jnp.bfloat16),
                dma, dma((4,)), dma((4,)), dma, dma, dma, dma, dma, dma, dma,
            ],
            compiler_params=pltpu.CompilerParams(collective_id=0, has_side_effects=True),
        )(particles, target_mean, precision.reshape(1, feat), low_factor)

    return jax.shard_map(local_steps, mesh=mesh, in_specs=(data_spec, mean_spec, prec_spec, factor_spec), out_specs=data_spec, check_vma=False)
```

```python
import functools

import jax
import jax.numpy as jnp
from jax import lax
from jax.experimental import pallas as pl
from jax.experimental.pallas import tpu as pltpu
from jax.sharding import PartitionSpec as P

NUM_STEPS = 3
SIDE = 4
CHIPS = SIDE ** 3
HALF = 128
MESH = pl.DeviceIdType.MESH
NT = (((1,), (1,)), ((), ()))


def _hops(offset):
    return sum(min(d, SIDE - d) for d in offset)


OFFSETS = sorted(
    [(a, b, c) for a in range(SIDE) for b in range(SIDE) for c in range(SIDE) if (a, b, c) != (0, 0, 0)],
    key=lambda offset: -_hops(offset),
)


def _kernel(consts, part_ref, mean_ref, prec_ref, factor_ref, out_ref,
            theta, spare, mean_own, mean_x, prec_own, prec_x, factor_own, factor_x, rs_send, rs_recv, gather, u_lo, u_hi,
            load_sem, swap_send, swap_recv, hello, go, rs_ssem, rs_rsem, ag_ssem, ag_rsem, back_send, back_recv):
    two_over_h, inv_h, step_size, inv_part = consts
    rank, feat = factor_ref.shape
    f32, bf16 = jnp.float32, jnp.bfloat16
    ens = lax.axis_index("ens")
    me = lax.axis_index("feat")
    core = me % 2
    chip = me // 2
    px, py, pz = chip % SIDE, (chip // SIDE) % SIDE, chip // (SIDE * SIDE)
    partner = chip * 2 + (1 - core)

    def peer(offset):
        dz, dy, dx = offset
        tz, ty, tx = (pz + dz) % SIDE, (py + dy) % SIDE, (px + dx) % SIDE
        return (tz * SIDE + ty) * SIDE + tx

    barrier = pltpu.get_barrier_semaphore()

    @pl.when(core == 0)
    def _():
        pl.semaphore_signal(barrier, inc=1, device_id=(ens, partner), device_id_type=MESH)

    loads = []
    for k, (src, dst) in enumerate((
        (part_ref.at[1 - core], spare), (part_ref.at[core], theta.at[:, pl.ds(0, feat)]),
        (mean_ref, mean_own), (prec_ref, prec_own), (factor_ref, factor_own),
    )):
        copy = pltpu.make_async_copy(src, dst, load_sem.at[k])
        copy.start()
        loads.append(copy)

    @pl.when(core == 1)
    def _():
        pl.semaphore_wait(barrier, 1)
        pl.semaphore_signal(hello, inc=1, device_id=(ens, partner), device_id_type=MESH)

    @pl.when(core == 0)
    def _():
        pl.semaphore_wait(hello, 1)
        for offset in OFFSETS:
            pl.semaphore_signal(barrier, inc=1, device_id=(ens, peer(offset) * 2), device_id_type=MESH)

    swaps = []
    for k, (load, src, dst) in enumerate((
        (loads[0], spare, theta.at[:, pl.ds(feat, feat)]), (loads[2], mean_own, mean_x),
        (loads[3], prec_own, prec_x), (loads[4], factor_own, factor_x),
    )):
        load.wait()
        copy = pltpu.make_async_remote_copy(src, dst, swap_send.at[k], swap_recv.at[k], device_id=(ens, partner), device_id_type=MESH)
        copy.start()
        swaps.append(copy)
    loads[1].wait()

    row_id = lax.broadcasted_iota(jnp.int32, (HALF, HALF), 0)
    col_id = lax.broadcasted_iota(jnp.int32, (HALF, HALF), 1)
    eye, upper = row_id == col_id, row_id <= col_id

    zeros = jnp.zeros((HALF - rank, 2 * feat), bf16)
    u_lo[rank:, :] = zeros
    u_hi[:HALF - rank, :] = zeros
    for copy in swaps:
        copy.wait_recv()
    factor = jnp.concatenate([factor_own[...], factor_x[...]], axis=1)
    u_lo[:rank, :] = factor
    u_hi[HALF - rank:, :] = factor
    mean_row = jnp.concatenate([mean_own[pl.ds(core, 1), :], mean_x[pl.ds(core, 1), :]], axis=1)
    prec_row = jnp.concatenate([prec_own[...], prec_x[...]], axis=1)
    others = pl.ds(0, CHIPS - 1)

    def drain(ref, sem):
        pltpu.make_async_copy(ref.at[others], ref.at[others], sem).wait()

    def partials():
        th = theta[...]
        tb = th.astype(bf16)
        xb = (th - mean_row).astype(bf16)
        top = lax.dot_general(tb[:HALF], tb, NT, preferred_element_type=f32)
        low = lax.dot_general(tb[HALF:], tb[HALF:], NT, preferred_element_type=f32)
        proj = (lax.dot_general(xb[:HALF], u_lo[...], NT, preferred_element_type=f32)
                + lax.dot_general(xb[HALF:], u_hi[...], NT, preferred_element_type=f32))
        tri = jnp.where(upper, top[:, :HALF], low)
        cross = top[:, HALF:]
        diag = jnp.sum(jnp.where(eye, low, 0.0), axis=0, keepdims=True)
        for o in range(CHIPS):
            block, r = (cross, 4 * o) if o < CHIPS // 2 else (tri, 4 * o - HALF)
            rs_send[o, 0:4, :] = block[r:r + 4]
            rs_send[o, 4:6, :] = proj[2 * o:2 * o + 2]
            rs_send[o, 6:7, :] = diag

    def all_reduce(first):
        for offset in OFFSETS:
            target = peer(offset)
            pltpu.make_async_remote_copy(
                rs_send.at[target], rs_recv.at[chip], rs_ssem, rs_rsem,
                device_id=(ens, target * 2 + core), device_id_type=MESH).start()
        rs_recv[chip] = rs_send[chip]
        if not first:
            drain(gather, ag_ssem)
        drain(rs_recv, rs_rsem)
        sums = [rs_recv[o] for o in range(4)]
        for o in range(4, CHIPS):
            sums[o % 4] = sums[o % 4] + rs_recv[o]
        total = (sums[0] + sums[1]) + (sums[2] + sums[3])
        gather[chip] = total[:6]
        for offset in OFFSETS:
            target = peer(offset)
            pltpu.make_async_remote_copy(
                gather.at[chip], gather.at[chip], ag_ssem, ag_rsem,
                device_id=(ens, target * 2 + core), device_id_type=MESH).start()
        drain(rs_send, rs_ssem)
        drain(gather, ag_rsem)
        return total[6:7]

    def update(diag, last):
        cross = jnp.concatenate([gather[o, 0:4, :] for o in range(CHIPS // 2)], axis=0)
        tri = jnp.concatenate([gather[o, 0:4, :] for o in range(CHIPS // 2, CHIPS)], axis=0)
        proj = jnp.concatenate([gather[o, 4:6, :] for o in range(CHIPS)], axis=0).astype(bf16)
        tri_t, cross_t = tri.T, cross.T
        g_aa = jnp.where(upper, tri, tri_t)
        g_cc = jnp.where(eye, diag, jnp.where(upper, tri_t, tri))
        row_a = jnp.sum(jnp.where(eye, tri, 0.0), axis=0, keepdims=True)
        col_a = jnp.sum(jnp.where(eye, tri, 0.0), axis=1, keepdims=True)
        col_c = jnp.sum(jnp.where(eye, diag, 0.0), axis=1, keepdims=True)
        top = jnp.concatenate([g_aa, cross], axis=1)
        bottom = jnp.concatenate([cross_t, g_cc], axis=1)
        row_all = jnp.concatenate([row_a, diag], axis=1)
        k_top = jnp.exp(-jnp.maximum(col_a + row_all - 2.0 * top, 0.0) * inv_h)
        k_bot = jnp.exp(-jnp.maximum(col_c + row_all - 2.0 * bottom, 0.0) * inv_h)
        kernel = jnp.concatenate([k_top, k_bot], axis=0)
        row_sum = jnp.sum(kernel, axis=1, keepdims=True)
        kernel_bf = kernel.astype(bf16)
        for part in (1, 0):
            cols = slice(part * feat, (part + 1) * feat)
            th = theta[:, cols]
            low = jnp.concatenate([
                jnp.dot(proj, u_lo[:, cols], preferred_element_type=f32),
                jnp.dot(proj, u_hi[:, cols], preferred_element_type=f32)], axis=0)
            grad = -((th - mean_row[:, cols]) * prec_row[:, cols] + low)
            mixed = (grad - two_over_h * th).astype(bf16)
            drive = jnp.dot(kernel_bf, mixed, preferred_element_type=f32)
            new = th + step_size * ((drive + two_over_h * row_sum * th) * inv_part)
            if not last:
                theta[:, cols] = new
            elif part == 1:
                spare[...] = new
                back = pltpu.make_async_remote_copy(
                    spare, out_ref.at[core], back_send, back_recv, device_id=(ens, partner), device_id_type=MESH)
                back.start()
            else:
                out_ref[core] = new

    partials()

    @pl.when(core == 0)
    def _():
        pl.semaphore_wait(barrier, CHIPS - 1)
        pl.semaphore_signal(go, inc=1, device_id=(ens, partner), device_id_type=MESH)

    @pl.when(core == 1)
    def _():
        pl.semaphore_wait(go, 1)

    first_diag = all_reduce(True)
    for copy in swaps:
        copy.wait_send()

    def body(_, diag):
        update(diag, False)
        partials()
        return all_reduce(False)

    update(lax.fori_loop(0, NUM_STEPS - 1, body, first_diag), True)
    drain(gather, ag_ssem)
    pltpu.make_async_remote_copy(
        spare, out_ref.at[1 - core], back_send, back_recv, device_id=(ens, partner), device_id_type=MESH).wait()


def solution(mesh):
    feat_count = mesh.shape["feat"]
    data_spec = P("ens", None, "feat")
    mean_spec = P("ens", "feat")
    prec_spec = P(("ens", "feat"))
    factor_spec = P(("ens", "feat"), None)

    def local_steps(particles, target_mean, precision, low_factor):
        _, num_part, feat = particles.shape
        rank = low_factor.shape[1]
        total_feat = feat * feat_count
        bandwidth = 2.0 * total_feat
        consts = (2.0 / bandwidth, 1.0 / bandwidth, 0.25 * total_feat, 1.0 / num_part)
        hbm, vmem = pl.BlockSpec(memory_space=pl.ANY), pl.BlockSpec(memory_space=pltpu.VMEM)
        dma, regular = pltpu.SemaphoreType.DMA, pltpu.SemaphoreType.REGULAR
        f32, bf16 = jnp.float32, jnp.bfloat16
        return pl.pallas_call(
            functools.partial(_kernel, consts),
            name="svgd",
            out_shape=pltpu.VMEM(particles.shape, f32),
            in_specs=[hbm, hbm, hbm, hbm],
            out_specs=vmem,
            scratch_shapes=[
                pltpu.VMEM((num_part, 2 * feat), f32),
                pltpu.VMEM((num_part, feat), f32),
                pltpu.VMEM((2, feat), f32),
                pltpu.VMEM((2, feat), f32),
                pltpu.VMEM((1, feat), f32),
                pltpu.VMEM((1, feat), f32),
                pltpu.VMEM((rank, feat), bf16),
                pltpu.VMEM((rank, feat), bf16),
                pltpu.VMEM((CHIPS, 7, HALF), f32),
                pltpu.VMEM((CHIPS, 7, HALF), f32),
                pltpu.VMEM((CHIPS, 6, HALF), f32),
                pltpu.VMEM((HALF, 2 * feat), bf16),
                pltpu.VMEM((HALF, 2 * feat), bf16),
                dma((5,)), dma((4,)), dma((4,)), regular, regular, dma, dma, dma, dma, dma, dma,
            ],
            compiler_params=pltpu.CompilerParams(collective_id=0, has_side_effects=True),
        )(particles, target_mean, precision.reshape(1, feat), low_factor.T)

    return jax.shard_map(local_steps, mesh=mesh, in_specs=(data_spec, mean_spec, prec_spec, factor_spec), out_specs=data_spec, check_vma=False)
```

```python
import functools

import jax
import jax.numpy as jnp
from jax import lax
from jax.experimental import pallas as pl
from jax.experimental.pallas import tpu as pltpu
from jax.sharding import PartitionSpec as P

NUM_STEPS = 3
SIDE = 4
CHIPS = SIDE ** 3
HALF = 128
MESH = pl.DeviceIdType.MESH
NT = (((1,), (1,)), ((), ()))


COST = (0, 7, 10, 7)
OFFSETS = sorted(
    [(a, b, c) for a in range(SIDE) for b in range(SIDE) for c in range(SIDE)],
    key=lambda offset: -sum(COST[d] for d in offset),
)


def _kernel(consts, part_ref, mean_ref, prec_ref, factor_ref, out_ref,
            theta, spare, mean_own, mean_x, prec_own, prec_x, factor_own, factor_x, rs_send, rs_recv, total, gather, u_lo, u_hi,
            load_sem, swap_send, swap_recv, hello, go, rs_ssem, rs_rsem, ag_ssem, ag_rsem, back_send, back_recv):
    two_over_h, inv_h, step_size, inv_part = consts
    rank, feat = factor_ref.shape
    f32, bf16 = jnp.float32, jnp.bfloat16
    ens = lax.axis_index("ens")
    me = lax.axis_index("feat")
    core = me % 2
    chip = me // 2
    px, py, pz = chip % SIDE, (chip // SIDE) % SIDE, chip // (SIDE * SIDE)
    partner = chip * 2 + (1 - core)

    def peer(offset):
        dz, dy, dx = offset
        tz, ty, tx = (pz + dz) % SIDE, (py + dy) % SIDE, (px + dx) % SIDE
        return (tz * SIDE + ty) * SIDE + tx

    barrier = pltpu.get_barrier_semaphore()

    @pl.when(core == 1)
    def _():
        pl.semaphore_signal(barrier, inc=1, device_id=(ens, partner), device_id_type=MESH)

    loads = []
    for k, (src, dst) in enumerate((
        (part_ref.at[1 - core], spare), (part_ref.at[core], theta.at[:, pl.ds(0, feat)]),
        (mean_ref, mean_own), (prec_ref, prec_own), (factor_ref, factor_own),
    )):
        copy = pltpu.make_async_copy(src, dst, load_sem.at[k])
        copy.start()
        loads.append(copy)

    @pl.when(core == 0)
    def _():
        pl.semaphore_wait(barrier, 1)
        pl.semaphore_signal(hello, inc=1, device_id=(ens, partner), device_id_type=MESH)

    @pl.when(core == 1)
    def _():
        pl.semaphore_wait(hello, 1)
        for offset in OFFSETS[:-1]:
            pl.semaphore_signal(barrier, inc=1, device_id=(ens, peer(offset) * 2 + 1), device_id_type=MESH)

    swaps = []
    for k, (load, src, dst) in enumerate((
        (loads[0], spare, theta.at[:, pl.ds(feat, feat)]), (loads[2], mean_own, mean_x),
        (loads[3], prec_own, prec_x), (loads[4], factor_own, factor_x),
    )):
        load.wait()
        copy = pltpu.make_async_remote_copy(src, dst, swap_send.at[k], swap_recv.at[k], device_id=(ens, partner), device_id_type=MESH)
        copy.start()
        swaps.append(copy)
    loads[1].wait()

    row_id = lax.broadcasted_iota(jnp.int32, (HALF, HALF), 0)
    col_id = lax.broadcasted_iota(jnp.int32, (HALF, HALF), 1)
    eye, upper = row_id == col_id, row_id <= col_id

    zeros = jnp.zeros((HALF - rank, 2 * feat), bf16)
    u_lo[rank:, :] = zeros
    u_hi[:HALF - rank, :] = zeros
    for copy in swaps:
        copy.wait_recv()
    factor = jnp.concatenate([factor_own[...], factor_x[...]], axis=1)
    u_lo[:rank, :] = factor
    u_hi[HALF - rank:, :] = factor
    mean_row = jnp.concatenate([mean_own[pl.ds(core, 1), :], mean_x[pl.ds(core, 1), :]], axis=1)
    prec_row = jnp.concatenate([prec_own[...], prec_x[...]], axis=1)

    def drain(ref, sem):
        pltpu.make_async_copy(ref, ref, sem).wait()

    def partials():
        th = theta[...]
        tb = th.astype(bf16)
        xb = (th - mean_row).astype(bf16)
        top = lax.dot_general(tb[:HALF], tb, NT, preferred_element_type=f32)
        low = lax.dot_general(tb[HALF:], tb[HALF:], NT, preferred_element_type=f32)
        proj = (lax.dot_general(xb[:HALF], u_lo[...], NT, preferred_element_type=f32)
                + lax.dot_general(xb[HALF:], u_hi[...], NT, preferred_element_type=f32))
        tri = jnp.where(upper, top[:, :HALF], low)
        cross = top[:, HALF:]
        diag = jnp.sum(jnp.where(eye, low, 0.0), axis=0, keepdims=True)
        for o in range(CHIPS):
            block, r = (cross, 4 * o) if o < CHIPS // 2 else (tri, 4 * o - HALF)
            rs_send[o, 0:4, :] = block[r:r + 4]
            rs_send[o, 4:6, :] = proj[2 * o:2 * o + 2]
            rs_send[o, 6:7, :] = diag

    def all_reduce(first):
        for offset in OFFSETS:
            target = peer(offset)
            pltpu.make_async_remote_copy(
                rs_send.at[target], rs_recv.at[chip], rs_ssem, rs_rsem,
                device_id=(ens, target * 2 + (1 - core)), device_id_type=MESH).start()
        if not first:
            drain(gather, ag_ssem)
        drain(rs_recv, rs_rsem)
        sums = [rs_recv[o] for o in range(4)]
        for o in range(4, CHIPS):
            sums[o % 4] = sums[o % 4] + rs_recv[o]
        total[...] = (sums[0] + sums[1]) + (sums[2] + sums[3])
        for offset in OFFSETS:
            target = peer(offset)
            pltpu.make_async_remote_copy(
                total, gather.at[chip], ag_ssem, ag_rsem,
                device_id=(ens, target * 2 + (1 - core)), device_id_type=MESH).start()
        drain(rs_send, rs_ssem)
        drain(gather, ag_rsem)

    def update(last):
        cross = jnp.concatenate([gather[o, 0:4, :] for o in range(CHIPS // 2)], axis=0)
        tri = jnp.concatenate([gather[o, 0:4, :] for o in range(CHIPS // 2, CHIPS)], axis=0)
        proj = jnp.concatenate([gather[o, 4:6, :] for o in range(CHIPS)], axis=0).astype(bf16)
        diag = gather[0, 6:7, :]
        tri_t, cross_t = tri.T, cross.T
        g_aa = jnp.where(upper, tri, tri_t)
        g_cc = jnp.where(eye, diag, jnp.where(upper, tri_t, tri))
        row_a = jnp.sum(jnp.where(eye, tri, 0.0), axis=0, keepdims=True)
        col_a = jnp.sum(jnp.where(eye, tri, 0.0), axis=1, keepdims=True)
        col_c = jnp.sum(jnp.where(eye, diag, 0.0), axis=1, keepdims=True)
        top = jnp.concatenate([g_aa, cross], axis=1)
        bottom = jnp.concatenate([cross_t, g_cc], axis=1)
        row_all = jnp.concatenate([row_a, diag], axis=1)
        k_top = jnp.exp(-jnp.maximum(col_a + row_all - 2.0 * top, 0.0) * inv_h)
        k_bot = jnp.exp(-jnp.maximum(col_c + row_all - 2.0 * bottom, 0.0) * inv_h)
        kernel = jnp.concatenate([k_top, k_bot], axis=0)
        row_sum = jnp.sum(kernel, axis=1, keepdims=True)
        kernel_bf = kernel.astype(bf16)
        for part in (1, 0):
            cols = slice(part * feat, (part + 1) * feat)
            th = theta[:, cols]
            low = jnp.concatenate([
                jnp.dot(proj, u_lo[:, cols], preferred_element_type=f32),
                jnp.dot(proj, u_hi[:, cols], preferred_element_type=f32)], axis=0)
            grad = -((th - mean_row[:, cols]) * prec_row[:, cols] + low)
            mixed = (grad - two_over_h * th).astype(bf16)
            drive = jnp.dot(kernel_bf, mixed, preferred_element_type=f32)
            new = th + step_size * ((drive + two_over_h * row_sum * th) * inv_part)
            if not last:
                theta[:, cols] = new
            elif part == 1:
                spare[...] = new
                back = pltpu.make_async_remote_copy(
                    spare, out_ref.at[core], back_send, back_recv, device_id=(ens, partner), device_id_type=MESH)
                back.start()
            else:
                out_ref[core] = new

    partials()

    @pl.when(core == 1)
    def _():
        pl.semaphore_wait(barrier, CHIPS - 1)
        pl.semaphore_signal(go, inc=1, device_id=(ens, partner), device_id_type=MESH)

    @pl.when(core == 0)
    def _():
        pl.semaphore_wait(go, 1)

    all_reduce(True)
    for copy in swaps:
        copy.wait_send()

    @pl.loop(0, NUM_STEPS - 1)
    def _(_):
        update(False)
        partials()
        all_reduce(False)

    update(True)
    drain(gather, ag_ssem)
    pltpu.make_async_remote_copy(
        spare, out_ref.at[1 - core], back_send, back_recv, device_id=(ens, partner), device_id_type=MESH).wait()


def solution(mesh):
    feat_count = mesh.shape["feat"]
    data_spec = P("ens", None, "feat")
    mean_spec = P("ens", "feat")
    prec_spec = P(("ens", "feat"))
    factor_spec = P(("ens", "feat"), None)

    def local_steps(particles, target_mean, precision, low_factor):
        _, num_part, feat = particles.shape
        rank = low_factor.shape[1]
        total_feat = feat * feat_count
        bandwidth = 2.0 * total_feat
        consts = (2.0 / bandwidth, 1.0 / bandwidth, 0.25 * total_feat, 1.0 / num_part)
        hbm, vmem = pl.BlockSpec(memory_space=pl.ANY), pl.BlockSpec(memory_space=pltpu.VMEM)
        dma, regular = pltpu.SemaphoreType.DMA, pltpu.SemaphoreType.REGULAR
        f32, bf16 = jnp.float32, jnp.bfloat16
        return pl.pallas_call(
            functools.partial(_kernel, consts),
            name="svgd",
            out_shape=pltpu.VMEM(particles.shape, f32),
            in_specs=[hbm, hbm, hbm, hbm],
            out_specs=vmem,
            scratch_shapes=[
                pltpu.VMEM((num_part, 2 * feat), f32),
                pltpu.VMEM((num_part, feat), f32),
                pltpu.VMEM((2, feat), f32),
                pltpu.VMEM((2, feat), f32),
                pltpu.VMEM((1, feat), f32),
                pltpu.VMEM((1, feat), f32),
                pltpu.VMEM((rank, feat), bf16),
                pltpu.VMEM((rank, feat), bf16),
                pltpu.VMEM((CHIPS, 7, HALF), f32),
                pltpu.VMEM((CHIPS, 7, HALF), f32),
                pltpu.VMEM((7, HALF), f32),
                pltpu.VMEM((CHIPS, 7, HALF), f32),
                pltpu.VMEM((HALF, 2 * feat), bf16),
                pltpu.VMEM((HALF, 2 * feat), bf16),
                dma((5,)), dma((4,)), dma((4,)), regular, regular, dma, dma, dma, dma, dma, dma,
            ],
            compiler_params=pltpu.CompilerParams(collective_id=0, has_side_effects=True),
        )(particles, target_mean, precision.reshape(1, feat), low_factor.T)

    return jax.shard_map(local_steps, mesh=mesh, in_specs=(data_spec, mean_spec, prec_spec, factor_spec), out_specs=data_spec, check_vma=False)
```

```python
import functools

import jax
import jax.numpy as jnp
from jax import lax
from jax.experimental import pallas as pl
from jax.experimental.pallas import tpu as pltpu
from jax.sharding import PartitionSpec as P

NUM_STEPS = 3
SIDE = 4
CHIPS = SIDE ** 3
HALF = 128
DIAG_CHIP = 21
MESH = pl.DeviceIdType.MESH
NT = (((1,), (1,)), ((), ()))


COST = (0, 7, 10, 7)
OFFSETS = sorted(
    [(a, b, c) for a in range(SIDE) for b in range(SIDE) for c in range(SIDE)],
    key=lambda offset: -sum(COST[d] for d in offset),
)


def _kernel(consts, part_ref, mean_ref, prec_ref, factor_ref, out_ref,
            theta, spare, mean_own, mean_x, prec_own, prec_x, factor_own, factor_x, rs_send, rs_recv, total, gather, diag_send, diag_recv, diag_total, diag_all, u_lo, u_hi,
            load_sem, swap_send, swap_recv, hello, go, rs_ssem, rs_rsem, ag_ssem, ag_rsem, dr_ssem, dr_rsem, dg_ssem, dg_rsem, back_send, back_recv):
    two_over_h, inv_h, step_size, inv_part = consts
    rank, feat = factor_ref.shape
    f32, bf16 = jnp.float32, jnp.bfloat16
    ens = lax.axis_index("ens")
    me = lax.axis_index("feat")
    core = me % 2
    chip = me // 2
    px, py, pz = chip % SIDE, (chip // SIDE) % SIDE, chip // (SIDE * SIDE)
    partner = chip * 2 + (1 - core)

    def peer(offset):
        dz, dy, dx = offset
        tz, ty, tx = (pz + dz) % SIDE, (py + dy) % SIDE, (px + dx) % SIDE
        return (tz * SIDE + ty) * SIDE + tx

    barrier = pltpu.get_barrier_semaphore()

    @pl.when(core == 1)
    def _():
        pl.semaphore_signal(barrier, inc=1, device_id=(ens, partner), device_id_type=MESH)

    loads = []
    for k, (src, dst) in enumerate((
        (part_ref.at[1 - core], spare), (part_ref.at[core], theta.at[:, pl.ds(0, feat)]),
        (mean_ref, mean_own), (prec_ref, prec_own), (factor_ref, factor_own),
    )):
        copy = pltpu.make_async_copy(src, dst, load_sem.at[k])
        copy.start()
        loads.append(copy)

    @pl.when(core == 0)
    def _():
        pl.semaphore_wait(barrier, 1)
        pl.semaphore_signal(hello, inc=1, device_id=(ens, partner), device_id_type=MESH)

    @pl.when(core == 1)
    def _():
        pl.semaphore_wait(hello, 1)
        for offset in OFFSETS[:-1]:
            pl.semaphore_signal(barrier, inc=1, device_id=(ens, peer(offset) * 2 + 1), device_id_type=MESH)

    swaps = []
    for k, (load, src, dst) in enumerate((
        (loads[0], spare, theta.at[:, pl.ds(feat, feat)]), (loads[2], mean_own, mean_x),
        (loads[3], prec_own, prec_x), (loads[4], factor_own, factor_x),
    )):
        load.wait()
        copy = pltpu.make_async_remote_copy(src, dst, swap_send.at[k], swap_recv.at[k], device_id=(ens, partner), device_id_type=MESH)
        copy.start()
        swaps.append(copy)
    loads[1].wait()

    row_id = lax.broadcasted_iota(jnp.int32, (HALF, HALF), 0)
    col_id = lax.broadcasted_iota(jnp.int32, (HALF, HALF), 1)
    eye, upper = row_id == col_id, row_id <= col_id

    zeros = jnp.zeros((HALF - rank, 2 * feat), bf16)
    u_lo[rank:, :] = zeros
    u_hi[:HALF - rank, :] = zeros
    for copy in swaps:
        copy.wait_recv()
    factor = jnp.concatenate([factor_own[...], factor_x[...]], axis=1)
    u_lo[:rank, :] = factor
    u_hi[HALF - rank:, :] = factor
    mean_row = jnp.concatenate([mean_own[pl.ds(core, 1), :], mean_x[pl.ds(core, 1), :]], axis=1)
    prec_row = jnp.concatenate([prec_own[...], prec_x[...]], axis=1)

    def drain(ref, sem):
        pltpu.make_async_copy(ref, ref, sem).wait()

    def partials():
        th = theta[...]
        tb = th.astype(bf16)
        xb = (th - mean_row).astype(bf16)
        top = lax.dot_general(tb[:HALF], tb, NT, preferred_element_type=f32)
        low = lax.dot_general(tb[HALF:], tb[HALF:], NT, preferred_element_type=f32)
        proj = (lax.dot_general(xb[:HALF], u_lo[...], NT, preferred_element_type=f32)
                + lax.dot_general(xb[HALF:], u_hi[...], NT, preferred_element_type=f32))
        tri = jnp.where(upper, top[:, :HALF], low)
        cross = top[:, HALF:]
        diag = jnp.sum(jnp.where(eye, low, 0.0), axis=0, keepdims=True)
        for o in range(CHIPS):
            block, r = (cross, 4 * o) if o < CHIPS // 2 else (tri, 4 * o - HALF)
            rs_send[o, 0:4, :] = block[r:r + 4]
            rs_send[o, 4:6, :] = proj[2 * o:2 * o + 2]
        diag_send[...] = diag

    def to_chip(src, dst, ssem, rsem, target):
        return pltpu.make_async_remote_copy(src, dst, ssem, rsem, device_id=(ens, target * 2 + (1 - core)), device_id_type=MESH)

    def all_reduce(first):
        diag_copy = to_chip(diag_send, diag_recv.at[chip], dr_ssem, dr_rsem, DIAG_CHIP)
        diag_copy.start()
        for offset in OFFSETS:
            target = peer(offset)
            to_chip(rs_send.at[target], rs_recv.at[chip], rs_ssem, rs_rsem, target).start()
        if not first:
            drain(gather, ag_ssem)
        drain(rs_recv, rs_rsem)
        sums = [rs_recv[o] for o in range(4)]
        for o in range(4, CHIPS):
            sums[o % 4] = sums[o % 4] + rs_recv[o]
        total[...] = (sums[0] + sums[1]) + (sums[2] + sums[3])

        @pl.when(chip == DIAG_CHIP)
        def _():
            drain(diag_recv, dr_rsem)
            diag = diag_recv[0]
            for o in range(1, CHIPS):
                diag = diag + diag_recv[o]
            diag_total[...] = diag
            for offset in OFFSETS:
                target = peer(offset)
                to_chip(diag_total, diag_all, dg_ssem, dg_rsem, target).start()
                to_chip(total, gather.at[chip], ag_ssem, ag_rsem, target).start()

        @pl.when(chip != DIAG_CHIP)
        def _():
            for offset in OFFSETS:
                to_chip(total, gather.at[chip], ag_ssem, ag_rsem, peer(offset)).start()

        drain(rs_send, rs_ssem)
        diag_copy.wait_send()
        drain(diag_all, dg_rsem)
        drain(gather, ag_rsem)

        @pl.when(chip == DIAG_CHIP)
        def _():
            drain(diag_recv, dg_ssem)

    def update(last):
        cross = jnp.concatenate([gather[o, 0:4, :] for o in range(CHIPS // 2)], axis=0)
        tri = jnp.concatenate([gather[o, 0:4, :] for o in range(CHIPS // 2, CHIPS)], axis=0)
        proj = jnp.concatenate([gather[o, 4:6, :] for o in range(CHIPS)], axis=0).astype(bf16)
        diag = diag_all[...]
        tri_t, cross_t = tri.T, cross.T
        g_aa = jnp.where(upper, tri, tri_t)
        g_cc = jnp.where(eye, diag, jnp.where(upper, tri_t, tri))
        row_a = jnp.sum(jnp.where(eye, tri, 0.0), axis=0, keepdims=True)
        col_a = jnp.sum(jnp.where(eye, tri, 0.0), axis=1, keepdims=True)
        col_c = jnp.sum(jnp.where(eye, diag, 0.0), axis=1, keepdims=True)
        top = jnp.concatenate([g_aa, cross], axis=1)
        bottom = jnp.concatenate([cross_t, g_cc], axis=1)
        row_all = jnp.concatenate([row_a, diag], axis=1)
        k_top = jnp.exp(-jnp.maximum(col_a + row_all - 2.0 * top, 0.0) * inv_h)
        k_bot = jnp.exp(-jnp.maximum(col_c + row_all - 2.0 * bottom, 0.0) * inv_h)
        kernel = jnp.concatenate([k_top, k_bot], axis=0)
        row_sum = jnp.sum(kernel, axis=1, keepdims=True)
        kernel_bf = kernel.astype(bf16)
        for part in (1, 0):
            cols = slice(part * feat, (part + 1) * feat)
            th = theta[:, cols]
            low = jnp.concatenate([
                jnp.dot(proj, u_lo[:, cols], preferred_element_type=f32),
                jnp.dot(proj, u_hi[:, cols], preferred_element_type=f32)], axis=0)
            grad = -((th - mean_row[:, cols]) * prec_row[:, cols] + low)
            mixed = (grad - two_over_h * th).astype(bf16)
            drive = jnp.dot(kernel_bf, mixed, preferred_element_type=f32)
            new = th + step_size * ((drive + two_over_h * row_sum * th) * inv_part)
            if not last:
                theta[:, cols] = new
            elif part == 1:
                spare[...] = new
                back = pltpu.make_async_remote_copy(
                    spare, out_ref.at[core], back_send, back_recv, device_id=(ens, partner), device_id_type=MESH)
                back.start()
            else:
                out_ref[core] = new

    partials()

    @pl.when(core == 1)
    def _():
        pl.semaphore_wait(barrier, CHIPS - 1)
        pl.semaphore_signal(go, inc=1, device_id=(ens, partner), device_id_type=MESH)

    @pl.when(core == 0)
    def _():
        pl.semaphore_wait(go, 1)

    all_reduce(True)
    for copy in swaps:
        copy.wait_send()

    @pl.loop(0, NUM_STEPS - 1)
    def _(_):
        update(False)
        partials()
        all_reduce(False)

    update(True)
    drain(gather, ag_ssem)
    pltpu.make_async_remote_copy(
        spare, out_ref.at[1 - core], back_send, back_recv, device_id=(ens, partner), device_id_type=MESH).wait()


def solution(mesh):
    feat_count = mesh.shape["feat"]
    data_spec = P("ens", None, "feat")
    mean_spec = P("ens", "feat")
    prec_spec = P(("ens", "feat"))
    factor_spec = P(("ens", "feat"), None)

    def local_steps(particles, target_mean, precision, low_factor):
        _, num_part, feat = particles.shape
        rank = low_factor.shape[1]
        total_feat = feat * feat_count
        bandwidth = 2.0 * total_feat
        consts = (2.0 / bandwidth, 1.0 / bandwidth, 0.25 * total_feat, 1.0 / num_part)
        hbm, vmem = pl.BlockSpec(memory_space=pl.ANY), pl.BlockSpec(memory_space=pltpu.VMEM)
        dma, regular = pltpu.SemaphoreType.DMA, pltpu.SemaphoreType.REGULAR
        f32, bf16 = jnp.float32, jnp.bfloat16
        return pl.pallas_call(
            functools.partial(_kernel, consts),
            name="svgd",
            out_shape=pltpu.VMEM(particles.shape, f32),
            in_specs=[hbm, hbm, hbm, hbm],
            out_specs=vmem,
            scratch_shapes=[
                pltpu.VMEM((num_part, 2 * feat), f32),
                pltpu.VMEM((num_part, feat), f32),
                pltpu.VMEM((2, feat), f32),
                pltpu.VMEM((2, feat), f32),
                pltpu.VMEM((1, feat), f32),
                pltpu.VMEM((1, feat), f32),
                pltpu.VMEM((rank, feat), bf16),
                pltpu.VMEM((rank, feat), bf16),
                pltpu.VMEM((CHIPS, 6, HALF), f32),
                pltpu.VMEM((CHIPS, 6, HALF), f32),
                pltpu.VMEM((6, HALF), f32),
                pltpu.VMEM((CHIPS, 6, HALF), f32),
                pltpu.VMEM((1, HALF), f32),
                pltpu.VMEM((CHIPS, 1, HALF), f32),
                pltpu.VMEM((1, HALF), f32),
                pltpu.VMEM((1, HALF), f32),
                pltpu.VMEM((HALF, 2 * feat), bf16),
                pltpu.VMEM((HALF, 2 * feat), bf16),
                dma((5,)), dma((4,)), dma((4,)), regular, regular, dma, dma, dma, dma, dma, dma, dma, dma, dma, dma,
            ],
            compiler_params=pltpu.CompilerParams(collective_id=0, has_side_effects=True),
        )(particles, target_mean, precision.reshape(1, feat), low_factor.T)

    return jax.shard_map(local_steps, mesh=mesh, in_specs=(data_spec, mean_spec, prec_spec, factor_spec), out_specs=data_spec, check_vma=False)
```

```python
import functools

import jax
import jax.numpy as jnp
from jax import lax
from jax.experimental import pallas as pl
from jax.experimental.pallas import tpu as pltpu
from jax.sharding import PartitionSpec as P

NUM_STEPS = 3
SIDE = 4
CHIPS = SIDE ** 3
HALF = 128
DIAG_CHIP = 21
EARLY = (0,)
MESH = pl.DeviceIdType.MESH
NT = (((1,), (1,)), ((), ()))


COST = (0, 7, 10, 7)
OFFSETS = sorted(
    [(a, b, c) for a in range(SIDE) for b in range(SIDE) for c in range(SIDE)],
    key=lambda offset: -sum(COST[d] for d in offset),
)


def _kernel(consts, part_ref, mean_ref, prec_ref, factor_ref, out_ref,
            theta, base, spare, mean_own, mean_x, prec_own, prec_x, factor_own, factor_x, rs_send, rs_recv, total, gather, diag_send, diag_recv, diag_total, diag_all, u_lo, u_hi,
            load_sem, swap_send, swap_recv, hello, go, rs_ssem, rs_rsem, ag_ssem, ag_rsem, dr_ssem, dr_rsem, dg_ssem, dg_rsem, ax_ssem, back_send, back_recv):
    two_over_h, inv_h, scale = consts
    rank, feat = factor_ref.shape
    f32, bf16 = jnp.float32, jnp.bfloat16
    ens = lax.axis_index("ens")
    me = lax.axis_index("feat")
    core = me % 2
    chip = me // 2
    px, py, pz = chip % SIDE, (chip // SIDE) % SIDE, chip // (SIDE * SIDE)
    partner = chip * 2 + (1 - core)

    def peer(offset):
        dz, dy, dx = offset
        tz, ty, tx = (pz + dz) % SIDE, (py + dy) % SIDE, (px + dx) % SIDE
        return (tz * SIDE + ty) * SIDE + tx

    barrier = pltpu.get_barrier_semaphore()

    loads = []
    for k, (src, dst) in enumerate((
        (part_ref.at[1 - core], spare), (part_ref.at[core], theta.at[:, pl.ds(0, feat)]),
        (mean_ref, mean_own), (prec_ref, prec_own), (factor_ref, factor_own),
    )):
        copy = pltpu.make_async_copy(src, dst, load_sem.at[k])
        copy.start()
        loads.append(copy)

    @pl.when(core == 1)
    def _():
        pl.semaphore_signal(barrier, inc=1, device_id=(ens, partner), device_id_type=MESH)
        for offset in OFFSETS[:-1]:
            pl.semaphore_signal(barrier, inc=1, device_id=(ens, peer(offset) * 2 + 1), device_id_type=MESH)
        pl.semaphore_wait(hello, 1)

    @pl.when(core == 0)
    def _():
        for offset in OFFSETS:
            pl.semaphore_signal(barrier, inc=1, device_id=(ens, peer(offset) * 2 + 1), device_id_type=MESH)
        pl.semaphore_wait(barrier, 1)
        pl.semaphore_signal(hello, inc=1, device_id=(ens, partner), device_id_type=MESH)

    swaps = []
    for k, (load, src, dst) in enumerate((
        (loads[0], spare, theta.at[:, pl.ds(feat, feat)]), (loads[2], mean_own, mean_x),
        (loads[3], prec_own, prec_x), (loads[4], factor_own, factor_x),
    )):
        load.wait()
        copy = pltpu.make_async_remote_copy(src, dst, swap_send.at[k], swap_recv.at[k], device_id=(ens, partner), device_id_type=MESH)
        copy.start()
        swaps.append(copy)
    loads[1].wait()

    row_id = lax.broadcasted_iota(jnp.int32, (HALF, HALF), 0)
    col_id = lax.broadcasted_iota(jnp.int32, (HALF, HALF), 1)
    eye, upper = row_id == col_id, row_id <= col_id

    zeros = jnp.zeros((HALF - rank, 2 * feat), bf16)
    u_lo[rank:, :] = zeros
    u_hi[:HALF - rank, :] = zeros
    for copy in swaps:
        copy.wait_recv()
    factor = jnp.concatenate([factor_own[...], factor_x[...]], axis=1)
    u_lo[:rank, :] = factor
    u_hi[HALF - rank:, :] = factor
    mean_row = jnp.concatenate([mean_own[pl.ds(core, 1), :], mean_x[pl.ds(core, 1), :]], axis=1)
    prec_row = jnp.concatenate([prec_own[...], prec_x[...]], axis=1)
    others = pl.ds(0, CHIPS - 1)

    def drain(ref, sem):
        pltpu.make_async_copy(ref, ref, sem).wait()

    def partials():
        th = theta[...]
        tb = th.astype(bf16)
        xb = (th - mean_row).astype(bf16)
        top = lax.dot_general(tb[:HALF], tb, NT, preferred_element_type=f32)
        low = lax.dot_general(tb[HALF:], tb[HALF:], NT, preferred_element_type=f32)
        proj = (lax.dot_general(xb[:HALF], u_lo[...], NT, preferred_element_type=f32)
                + lax.dot_general(xb[HALF:], u_hi[...], NT, preferred_element_type=f32))
        tri = jnp.where(upper, top[:, :HALF], low)
        cross = top[:, HALF:]
        diag = jnp.sum(jnp.where(eye, low, 0.0), axis=0, keepdims=True)
        for o in range(CHIPS):
            block, r = (cross, 4 * o) if o < CHIPS // 2 else (tri, 4 * o - HALF)
            rs_send[o, 0:4, :] = block[r:r + 4]
            rs_send[o, 4:6, :] = proj[2 * o:2 * o + 2]
        diag_send[...] = diag

    def to_core(src, dst, ssem, rsem, target, on):
        return pltpu.make_async_remote_copy(src, dst, ssem, rsem, device_id=(ens, target * 2 + on), device_id_type=MESH)

    other = 1 - core

    def scatter():
        to_core(diag_send, diag_recv.at[chip], dr_ssem, dr_rsem, DIAG_CHIP, other).start()
        for offset in OFFSETS:
            target = peer(offset)
            to_core(rs_send.at[target], rs_recv.at[chip], rs_ssem, rs_rsem, target, other).start()

    def reduce():
        drain(rs_recv, rs_rsem)
        sums = [rs_recv[o] for o in range(4)]
        for o in range(4, CHIPS):
            sums[o % 4] = sums[o % 4] + rs_recv[o]
        total[...] = (sums[0] + sums[1]) + (sums[2] + sums[3])

    def reduce_diag():
        drain(diag_recv, dr_rsem)
        sums = [diag_recv[o] for o in range(4)]
        for o in range(4, CHIPS):
            sums[o % 4] = sums[o % 4] + diag_recv[o]
        diag_total[...] = (sums[0] + sums[1]) + (sums[2] + sums[3])

    def all_gather(last):
        @pl.when(chip == DIAG_CHIP)
        def _():
            reduce_diag()
            if last:
                for target in EARLY:
                    to_core(diag_total, diag_all.at[1], dg_ssem, dg_rsem.at[1], target, core).start()
            for offset in OFFSETS:
                to_core(diag_total, diag_all.at[0], dg_ssem, dg_rsem.at[0], peer(offset), other).start()

        if last:
            for target in EARLY:
                @pl.when(chip != target)
                def _():
                    to_core(total, gather.at[1, chip], ax_ssem, ag_rsem.at[1], target, core).start()
        for offset in OFFSETS:
            to_core(total, gather.at[0, chip], ag_ssem, ag_rsem.at[0], peer(offset), other).start()
        drain(rs_send, rs_ssem)
        drain(diag_send, dr_ssem)

    def sent(last):
        drain(gather.at[0], ag_ssem)

        @pl.when(chip == DIAG_CHIP)
        def _():
            drain(diag_recv, dg_ssem)
            if last:
                drain(diag_recv.at[pl.ds(0, len(EARLY))], dg_ssem)

        if last:
            drain(gather.at[1, pl.ds(0, len(EARLY) - 1)], ax_ssem) if len(EARLY) > 1 else None

            @pl.when(jnp.logical_not(early))
            def _():
                drain(total, ax_ssem)

    def kernel_matrix(k):
        diag = diag_all[k]
        cross = jnp.concatenate([gather[k, o, 0:4, :] for o in range(CHIPS // 2)], axis=0)
        tri = jnp.concatenate([gather[k, o, 0:4, :] for o in range(CHIPS // 2, CHIPS)], axis=0)
        proj = jnp.concatenate([gather[k, o, 4:6, :] for o in range(CHIPS)], axis=0).astype(bf16)
        tri_t, cross_t = tri.T, cross.T
        g_aa = jnp.where(upper, tri, tri_t)
        g_cc = jnp.where(eye, diag, jnp.where(upper, tri_t, tri))
        row_a = jnp.sum(jnp.where(eye, tri, 0.0), axis=0, keepdims=True)
        col_a = jnp.sum(jnp.where(eye, tri, 0.0), axis=1, keepdims=True)
        col_c = jnp.sum(jnp.where(eye, diag, 0.0), axis=1, keepdims=True)
        top = jnp.concatenate([g_aa, cross], axis=1)
        bottom = jnp.concatenate([cross_t, g_cc], axis=1)
        row_all = jnp.concatenate([row_a, diag], axis=1)
        k_top = jnp.exp(-jnp.maximum(col_a + row_all - 2.0 * top, 0.0) * inv_h)
        k_bot = jnp.exp(-jnp.maximum(col_c + row_all - 2.0 * bottom, 0.0) * inv_h)
        kernel = jnp.concatenate([k_top, k_bot], axis=0)
        keep = 1.0 + (scale * two_over_h) * jnp.sum(kernel, axis=1, keepdims=True)
        return kernel.astype(bf16), keep, proj

    def moved(kernel_bf, keep, proj, th, still, cols):
        low = jnp.concatenate([
            jnp.dot(proj, u_lo[:, cols], preferred_element_type=f32),
            jnp.dot(proj, u_hi[:, cols], preferred_element_type=f32)], axis=0)
        drive = jnp.dot(kernel_bf, (still - low).astype(bf16), preferred_element_type=f32)
        return keep * th + scale * drive

    own = slice(0, feat)
    early = functools.reduce(jnp.logical_or, [chip == target for target in EARLY])
    partials()
    for copy in swaps:
        copy.wait_send()

    @pl.when(core == 1)
    def _():
        pl.semaphore_wait(barrier, 2 * CHIPS - 1)
        pl.semaphore_signal(go, inc=1, device_id=(ens, partner), device_id_type=MESH)

    @pl.when(core == 0)
    def _():
        pl.semaphore_wait(go, 1)

    @pl.loop(0, NUM_STEPS - 1)
    def _(_):
        scatter()
        base[...] = -((theta[...] - mean_row) * prec_row) - two_over_h * theta[...]
        reduce()
        all_gather(False)
        drain(diag_all.at[0], dg_rsem.at[0])
        drain(gather.at[0], ag_rsem.at[0])
        weights = kernel_matrix(0)
        for part in range(2):
            cols = slice(part * feat, (part + 1) * feat)
            theta[:, cols] = moved(*weights, theta[:, cols], base[:, cols], cols)
        partials()
        sent(False)

    def still(th, mean, prec):
        return -((th - mean) * prec) - two_over_h * th

    scatter()

    def back_copy(src, dst):
        return pltpu.make_async_remote_copy(src, dst, back_send, back_recv, device_id=(ens, partner), device_id_type=MESH)

    @pl.when(early)
    def _():
        back = back_copy(theta.at[:, pl.ds(feat, feat)], spare)
        back.start()
        base[:, own] = still(theta[:, own], mean_own[pl.ds(core, 1), :], prec_own[...])
        back.wait()
        base[:, feat:] = still(spare[...], mean_own[pl.ds(other, 1), :], prec_own[...])

    @pl.when(jnp.logical_not(early))
    def _():
        base[...] = still(theta[...], mean_row, prec_row)

    reduce()
    all_gather(True)
    drain(diag_all.at[0], dg_rsem.at[0])
    drain(gather.at[0], ag_rsem.at[0])

    @pl.when(early)
    def _():
        out_ref[core] = moved(*kernel_matrix(0), theta[:, own], base[:, own], own)
        gather[1, chip] = total[...]
        drain(diag_all.at[1], dg_rsem.at[1])
        drain(gather.at[1, others], ag_rsem.at[1])
        out_ref[other] = moved(*kernel_matrix(1), spare[...], base[:, feat:], own)

    @pl.when(jnp.logical_not(early))
    def _():
        weights = kernel_matrix(0)
        spare[...] = moved(*weights, theta[:, feat:], base[:, feat:], slice(feat, 2 * feat))
        back_copy(spare, out_ref.at[core]).start()
        out_ref[core] = moved(*weights, theta[:, own], base[:, own], own)
        back_copy(spare, out_ref.at[other]).wait()

    sent(True)


def solution(mesh):
    feat_count = mesh.shape["feat"]
    data_spec = P("ens", None, "feat")
    mean_spec = P("ens", "feat")
    prec_spec = P(("ens", "feat"))
    factor_spec = P(("ens", "feat"), None)

    def local_steps(particles, target_mean, precision, low_factor):
        _, num_part, feat = particles.shape
        rank = low_factor.shape[1]
        total_feat = feat * feat_count
        bandwidth = 2.0 * total_feat
        consts = (2.0 / bandwidth, 1.0 / bandwidth, 0.25 * total_feat / num_part)
        hbm, vmem = pl.BlockSpec(memory_space=pl.ANY), pl.BlockSpec(memory_space=pltpu.VMEM)
        dma, regular = pltpu.SemaphoreType.DMA, pltpu.SemaphoreType.REGULAR
        f32, bf16 = jnp.float32, jnp.bfloat16
        return pl.pallas_call(
            functools.partial(_kernel, consts),
            name="svgd",
            out_shape=pltpu.VMEM(particles.shape, f32),
            in_specs=[hbm, hbm, hbm, hbm],
            out_specs=vmem,
            scratch_shapes=[
                pltpu.VMEM((num_part, 2 * feat), f32),
                pltpu.VMEM((num_part, 2 * feat), f32),
                pltpu.VMEM((num_part, feat), f32),
                pltpu.VMEM((2, feat), f32),
                pltpu.VMEM((2, feat), f32),
                pltpu.VMEM((1, feat), f32),
                pltpu.VMEM((1, feat), f32),
                pltpu.VMEM((rank, feat), bf16),
                pltpu.VMEM((rank, feat), bf16),
                pltpu.VMEM((CHIPS, 6, HALF), f32),
                pltpu.VMEM((CHIPS, 6, HALF), f32),
                pltpu.VMEM((6, HALF), f32),
                pltpu.VMEM((2, CHIPS, 6, HALF), f32),
                pltpu.VMEM((1, HALF), f32),
                pltpu.VMEM((CHIPS, 1, HALF), f32),
                pltpu.VMEM((1, HALF), f32),
                pltpu.VMEM((2, 1, HALF), f32),
                pltpu.VMEM((HALF, 2 * feat), bf16),
                pltpu.VMEM((HALF, 2 * feat), bf16),
                dma((5,)), dma((4,)), dma((4,)), regular, regular, dma, dma, dma, dma((2,)), dma, dma, dma, dma((2,)), dma, dma, dma,
            ],
            compiler_params=pltpu.CompilerParams(collective_id=0, has_side_effects=True),
        )(particles, target_mean, precision.reshape(1, feat), low_factor.T)

    return jax.shard_map(local_steps, mesh=mesh, in_specs=(data_spec, mean_spec, prec_spec, factor_spec), out_specs=data_spec, check_vma=False)
```

```python
import functools

import jax
import jax.numpy as jnp
from jax import lax
from jax.experimental import pallas as pl
from jax.experimental.pallas import tpu as pltpu
from jax.sharding import PartitionSpec as P

NUM_STEPS = 3
SIDE = 4
CHIPS = SIDE ** 3
HALF = 128
DIAG_CHIP = 21
EARLY = (0,)
LAG = 600
MESH = pl.DeviceIdType.MESH
NT = (((1,), (1,)), ((), ()))


COST = (0, 7, 10, 7)
OFFSETS = sorted(
    [(a, b, c) for a in range(SIDE) for b in range(SIDE) for c in range(SIDE)],
    key=lambda offset: -sum(COST[d] for d in offset),
)


def _kernel(consts, part_ref, mean_ref, prec_ref, factor_ref, out_ref,
            theta, base, spare, mean_own, mean_x, prec_own, prec_x, factor_own, factor_x, rs_send, rs_recv, total, gather, diag_send, diag_recv, diag_total, diag_all, u_lo, u_hi,
            load_sem, swap_send, swap_recv, hello, go, rs_ssem, rs_rsem, ag_ssem, ag_rsem, dr_ssem, dr_rsem, dg_ssem, dg_rsem, ax_ssem, back_send, back_recv):
    two_over_h, inv_h, scale = consts
    rank, feat = factor_ref.shape
    num_part = part_ref.shape[1]
    f32, bf16 = jnp.float32, jnp.bfloat16
    ens = lax.axis_index("ens")
    me = lax.axis_index("feat")
    core = me % 2
    chip = me // 2
    px, py, pz = chip % SIDE, (chip // SIDE) % SIDE, chip // (SIDE * SIDE)
    partner = chip * 2 + (1 - core)

    def peer(offset):
        dz, dy, dx = offset
        tz, ty, tx = (pz + dz) % SIDE, (py + dy) % SIDE, (px + dx) % SIDE
        return (tz * SIDE + ty) * SIDE + tx

    barrier = pltpu.get_barrier_semaphore()

    loads = []
    for k, (src, dst) in enumerate((
        (part_ref.at[1 - core], spare), (part_ref.at[core], theta.at[:, pl.ds(0, feat)]),
        (mean_ref, mean_own), (prec_ref, prec_own), (factor_ref, factor_own),
    )):
        copy = pltpu.make_async_copy(src, dst, load_sem.at[k])
        copy.start()
        loads.append(copy)

    @pl.when(core == 1)
    def _():
        pl.semaphore_signal(barrier, inc=1, device_id=(ens, partner), device_id_type=MESH)
        for offset in OFFSETS[:-1]:
            pl.semaphore_signal(barrier, inc=1, device_id=(ens, peer(offset) * 2 + 1), device_id_type=MESH)
        pl.semaphore_wait(hello, 1)

    @pl.when(core == 0)
    def _():
        for offset in OFFSETS:
            pl.semaphore_signal(barrier, inc=1, device_id=(ens, peer(offset) * 2 + 1), device_id_type=MESH)
        pl.semaphore_wait(barrier, 1)
        pl.semaphore_signal(hello, inc=1, device_id=(ens, partner), device_id_type=MESH)

    swaps = []
    for k, (load, src, dst) in enumerate((
        (loads[0], spare, theta.at[:, pl.ds(feat, feat)]), (loads[2], mean_own, mean_x),
        (loads[3], prec_own, prec_x), (loads[4], factor_own, factor_x),
    )):
        load.wait()
        copy = pltpu.make_async_remote_copy(src, dst, swap_send.at[k], swap_recv.at[k], device_id=(ens, partner), device_id_type=MESH)
        copy.start()
        swaps.append(copy)
    loads[1].wait()

    row_id = lax.broadcasted_iota(jnp.int32, (HALF, HALF), 0)
    col_id = lax.broadcasted_iota(jnp.int32, (HALF, HALF), 1)
    eye, upper = row_id == col_id, row_id <= col_id

    zeros = jnp.zeros((HALF - rank, 2 * feat), bf16)
    u_lo[rank:, :] = zeros
    u_hi[:HALF - rank, :] = zeros
    for copy in swaps:
        copy.wait_recv()
    factor = jnp.concatenate([factor_own[...], factor_x[...]], axis=1)
    u_lo[:rank, :] = factor
    u_hi[HALF - rank:, :] = factor
    mean_row = jnp.concatenate([mean_own[pl.ds(core, 1), :], mean_x[pl.ds(core, 1), :]], axis=1)
    prec_row = jnp.concatenate([prec_own[...], prec_x[...]], axis=1)
    others = pl.ds(0, CHIPS - 1)

    def drain(ref, sem):
        pltpu.make_async_copy(ref, ref, sem).wait()

    def partials():
        th = theta[...]
        tb = th.astype(bf16)
        xb = (th - mean_row).astype(bf16)
        top = lax.dot_general(tb[:HALF], tb, NT, preferred_element_type=f32)
        low = lax.dot_general(tb[HALF:], tb[HALF:], NT, preferred_element_type=f32)
        proj = (lax.dot_general(xb[:HALF], u_lo[...], NT, preferred_element_type=f32)
                + lax.dot_general(xb[HALF:], u_hi[...], NT, preferred_element_type=f32))
        tri = jnp.where(upper, top[:, :HALF], low)
        cross = top[:, HALF:]
        diag = jnp.sum(jnp.where(eye, low, 0.0), axis=0, keepdims=True)
        for o in range(CHIPS):
            block, r = (cross, 4 * o) if o < CHIPS // 2 else (tri, 4 * o - HALF)
            rs_send[o, 0:4, :] = block[r:r + 4]
            rs_send[o, 4:6, :] = proj[2 * o:2 * o + 2]
        diag_send[...] = diag

    def to_core(src, dst, ssem, rsem, target, on):
        return pltpu.make_async_remote_copy(src, dst, ssem, rsem, device_id=(ens, target * 2 + on), device_id_type=MESH)

    other = 1 - core

    def scatter():
        to_core(diag_send, diag_recv.at[chip], dr_ssem, dr_rsem, DIAG_CHIP, other).start()
        for offset in OFFSETS:
            target = peer(offset)
            to_core(rs_send.at[target], rs_recv.at[chip], rs_ssem, rs_rsem, target, other).start()

    def reduce():
        drain(rs_recv, rs_rsem)
        sums = [rs_recv[o] for o in range(4)]
        for o in range(4, CHIPS):
            sums[o % 4] = sums[o % 4] + rs_recv[o]
        total[...] = (sums[0] + sums[1]) + (sums[2] + sums[3])

    def reduce_diag():
        drain(diag_recv, dr_rsem)
        sums = [diag_recv[o] for o in range(4)]
        for o in range(4, CHIPS):
            sums[o % 4] = sums[o % 4] + diag_recv[o]
        diag_total[...] = (sums[0] + sums[1]) + (sums[2] + sums[3])

    def all_gather(last):
        @pl.when(chip == DIAG_CHIP)
        def _():
            reduce_diag()
            if last:
                for target in EARLY:
                    to_core(diag_total, diag_all.at[1], dg_ssem, dg_rsem.at[1], target, core).start()
            for offset in OFFSETS:
                to_core(diag_total, diag_all.at[0], dg_ssem, dg_rsem.at[0], peer(offset), other).start()

        if last:
            for target in EARLY:
                @pl.when(chip != target)
                def _():
                    to_core(total, gather.at[1, chip], ax_ssem, ag_rsem.at[1], target, core).start()
        for offset in OFFSETS:
            to_core(total, gather.at[0, chip], ag_ssem, ag_rsem.at[0], peer(offset), other).start()
        drain(rs_send, rs_ssem)
        drain(diag_send, dr_ssem)

    def sent(last):
        drain(gather.at[0], ag_ssem)

        @pl.when(chip == DIAG_CHIP)
        def _():
            drain(diag_recv, dg_ssem)
            if last:
                drain(diag_recv.at[pl.ds(0, len(EARLY))], dg_ssem)

        if last:
            drain(gather.at[1, pl.ds(0, len(EARLY) - 1)], ax_ssem) if len(EARLY) > 1 else None

            @pl.when(jnp.logical_not(early))
            def _():
                drain(total, ax_ssem)

    def kernel_matrix(k):
        diag = diag_all[k]
        cross = jnp.concatenate([gather[k, o, 0:4, :] for o in range(CHIPS // 2)], axis=0)
        tri = jnp.concatenate([gather[k, o, 0:4, :] for o in range(CHIPS // 2, CHIPS)], axis=0)
        proj = jnp.concatenate([gather[k, o, 4:6, :] for o in range(CHIPS)], axis=0).astype(bf16)
        tri_t, cross_t = tri.T, cross.T
        g_aa = jnp.where(upper, tri, tri_t)
        g_cc = jnp.where(eye, diag, jnp.where(upper, tri_t, tri))
        row_a = jnp.sum(jnp.where(eye, tri, 0.0), axis=0, keepdims=True)
        col_a = jnp.sum(jnp.where(eye, tri, 0.0), axis=1, keepdims=True)
        col_c = jnp.sum(jnp.where(eye, diag, 0.0), axis=1, keepdims=True)
        top = jnp.concatenate([g_aa, cross], axis=1)
        bottom = jnp.concatenate([cross_t, g_cc], axis=1)
        row_all = jnp.concatenate([row_a, diag], axis=1)
        k_top = jnp.exp(-jnp.maximum(col_a + row_all - 2.0 * top, 0.0) * inv_h)
        k_bot = jnp.exp(-jnp.maximum(col_c + row_all - 2.0 * bottom, 0.0) * inv_h)
        kernel = jnp.concatenate([k_top, k_bot], axis=0)
        keep = 1.0 + (scale * two_over_h) * jnp.sum(kernel, axis=1, keepdims=True)
        return kernel.astype(bf16), keep, proj

    def mixed(proj, still, cols):
        low = jnp.concatenate([
            jnp.dot(proj, u_lo[:, cols], preferred_element_type=f32),
            jnp.dot(proj, u_hi[:, cols], preferred_element_type=f32)], axis=0)
        return (still - low).astype(bf16)

    def moved(kernel_bf, keep, proj, th, still, cols):
        return keep * th + scale * jnp.dot(kernel_bf, mixed(proj, still, cols), preferred_element_type=f32)

    own = slice(0, feat)
    early = functools.reduce(jnp.logical_or, [chip == target for target in EARLY])
    partials()
    for copy in swaps:
        copy.wait_send()

    @pl.when(core == 1)
    def _():
        pl.semaphore_wait(barrier, 2 * CHIPS - 1)
        pl.semaphore_signal(go, inc=1, device_id=(ens, partner), device_id_type=MESH)

    @pl.when(core == 0)
    def _():
        pl.semaphore_wait(go, 1)

    @pl.when(core == 0)
    def _():
        pl.delay(LAG)

    @pl.loop(0, NUM_STEPS - 1)
    def _(_):
        scatter()
        base[...] = -((theta[...] - mean_row) * prec_row) - two_over_h * theta[...]
        reduce()
        all_gather(False)
        drain(diag_all.at[0], dg_rsem.at[0])
        drain(gather.at[0], ag_rsem.at[0])
        weights = kernel_matrix(0)
        for part in range(2):
            cols = slice(part * feat, (part + 1) * feat)
            theta[:, cols] = moved(*weights, theta[:, cols], base[:, cols], cols)
        partials()
        sent(False)

    def still(th, mean, prec):
        return -((th - mean) * prec) - two_over_h * th

    scatter()

    def back_copy(src, dst):
        return pltpu.make_async_remote_copy(src, dst, back_send, back_recv, device_id=(ens, partner), device_id_type=MESH)

    @pl.when(early)
    def _():
        back = back_copy(theta.at[:, pl.ds(feat, feat)], spare)
        back.start()
        base[:, own] = still(theta[:, own], mean_own[pl.ds(core, 1), :], prec_own[...])
        back.wait()
        base[:, feat:] = still(spare[...], mean_own[pl.ds(other, 1), :], prec_own[...])

    @pl.when(jnp.logical_not(early))
    def _():
        base[...] = still(theta[...], mean_row, prec_row)

    reduce()
    all_gather(True)
    drain(diag_all.at[0], dg_rsem.at[0])
    drain(gather.at[0], ag_rsem.at[0])

    @pl.when(early)
    def _():
        out_ref[core] = moved(*kernel_matrix(0), theta[:, own], base[:, own], own)
        gather[1, chip] = total[...]
        drain(diag_all.at[1], dg_rsem.at[1])
        drain(gather.at[1, others], ag_rsem.at[1])
        out_ref[other] = moved(*kernel_matrix(1), spare[...], base[:, feat:], own)

    @pl.when(jnp.logical_not(early))
    def _():
        weights = kernel_matrix(0)
        kernel_bf, keep, proj = weights
        partners = mixed(proj, base[:, feat:], slice(feat, 2 * feat))
        step = num_part // 2
        for r in range(0, num_part, step):
            rows = slice(r, r + step)
            spare[rows] = keep[rows] * theta[rows, feat:] + scale * jnp.dot(kernel_bf[rows], partners, preferred_element_type=f32)
            back_copy(spare.at[pl.ds(r, step)], out_ref.at[core, pl.ds(r, step)]).start()
        out_ref[core] = moved(*weights, theta[:, own], base[:, own], own)
        back_copy(spare, out_ref.at[other]).wait()

    sent(True)


def solution(mesh):
    feat_count = mesh.shape["feat"]
    data_spec = P("ens", None, "feat")
    mean_spec = P("ens", "feat")
    prec_spec = P(("ens", "feat"))
    factor_spec = P(("ens", "feat"), None)

    def local_steps(particles, target_mean, precision, low_factor):
        _, num_part, feat = particles.shape
        rank = low_factor.shape[1]
        total_feat = feat * feat_count
        bandwidth = 2.0 * total_feat
        consts = (2.0 / bandwidth, 1.0 / bandwidth, 0.25 * total_feat / num_part)
        hbm, vmem = pl.BlockSpec(memory_space=pl.ANY), pl.BlockSpec(memory_space=pltpu.VMEM)
        dma, regular = pltpu.SemaphoreType.DMA, pltpu.SemaphoreType.REGULAR
        f32, bf16 = jnp.float32, jnp.bfloat16
        return pl.pallas_call(
            functools.partial(_kernel, consts),
            name="svgd",
            out_shape=pltpu.VMEM(particles.shape, f32),
            in_specs=[hbm, hbm, hbm, hbm],
            out_specs=vmem,
            scratch_shapes=[
                pltpu.VMEM((num_part, 2 * feat), f32),
                pltpu.VMEM((num_part, 2 * feat), f32),
                pltpu.VMEM((num_part, feat), f32),
                pltpu.VMEM((2, feat), f32),
                pltpu.VMEM((2, feat), f32),
                pltpu.VMEM((1, feat), f32),
                pltpu.VMEM((1, feat), f32),
                pltpu.VMEM((rank, feat), bf16),
                pltpu.VMEM((rank, feat), bf16),
                pltpu.VMEM((CHIPS, 6, HALF), f32),
                pltpu.VMEM((CHIPS, 6, HALF), f32),
                pltpu.VMEM((6, HALF), f32),
                pltpu.VMEM((2, CHIPS, 6, HALF), f32),
                pltpu.VMEM((1, HALF), f32),
                pltpu.VMEM((CHIPS, 1, HALF), f32),
                pltpu.VMEM((1, HALF), f32),
                pltpu.VMEM((2, 1, HALF), f32),
                pltpu.VMEM((HALF, 2 * feat), bf16),
                pltpu.VMEM((HALF, 2 * feat), bf16),
                dma((5,)), dma((4,)), dma((4,)), regular, regular, dma, dma, dma, dma((2,)), dma, dma, dma, dma((2,)), dma, dma, dma,
            ],
            compiler_params=pltpu.CompilerParams(collective_id=0, has_side_effects=True),
        )(particles, target_mean, precision.reshape(1, feat), low_factor.T)

    return jax.shard_map(local_steps, mesh=mesh, in_specs=(data_spec, mean_spec, prec_spec, factor_spec), out_specs=data_spec, check_vma=False)
```

```python
import functools

import jax
import jax.numpy as jnp
from jax import lax
from jax.experimental import pallas as pl
from jax.experimental.pallas import tpu as pltpu
from jax.sharding import PartitionSpec as P

NUM_STEPS = 3
SIDE = 4
CHIPS = SIDE ** 3
HALF = 128
DIAG_CHIP = 21
EARLY = (0,)
LAG = 600
MESH = pl.DeviceIdType.MESH
NT = (((1,), (1,)), ((), ()))


COST = (0, 7, 10, 7)
OFFSETS = sorted(
    [(a, b, c) for a in range(SIDE) for b in range(SIDE) for c in range(SIDE)],
    key=lambda offset: -sum(COST[d] for d in offset),
)


def _kernel(consts, part_ref, mean_ref, prec_ref, factor_ref, out_ref,
            theta, base, spare, mean_own, mean_x, prec_own, prec_x, factor_own, factor_x, rs_send, rs_recv, total, gather, diag_send, diag_recv, diag_total, diag_all, u_lo, u_hi,
            load_sem, swap_send, swap_recv, hello, go, rs_ssem, rs_rsem, ag_ssem, ag_rsem, dr_ssem, dr_rsem, dg_ssem, dg_rsem, ax_ssem, back_send, back_recv):
    two_over_h, inv_h, scale = consts
    rank, feat = factor_ref.shape
    num_part = part_ref.shape[1]
    f32, bf16 = jnp.float32, jnp.bfloat16
    ens = lax.axis_index("ens")
    me = lax.axis_index("feat")
    core = me % 2
    chip = me // 2
    px, py, pz = chip % SIDE, (chip // SIDE) % SIDE, chip // (SIDE * SIDE)
    partner = chip * 2 + (1 - core)

    def peer(offset):
        dz, dy, dx = offset
        tz, ty, tx = (pz + dz) % SIDE, (py + dy) % SIDE, (px + dx) % SIDE
        return (tz * SIDE + ty) * SIDE + tx

    barrier = pltpu.get_barrier_semaphore()

    loads = []
    for k, (src, dst) in enumerate((
        (part_ref.at[1 - core], spare), (part_ref.at[core], theta.at[:, pl.ds(0, feat)]),
        (mean_ref, mean_own), (prec_ref, prec_own), (factor_ref, factor_own),
    )):
        copy = pltpu.make_async_copy(src, dst, load_sem.at[k])
        copy.start()
        loads.append(copy)

    @pl.when(core == 1)
    def _():
        pl.semaphore_signal(barrier, inc=1, device_id=(ens, partner), device_id_type=MESH)
        for offset in OFFSETS[:-1]:
            pl.semaphore_signal(barrier, inc=1, device_id=(ens, peer(offset) * 2 + 1), device_id_type=MESH)
        pl.semaphore_wait(hello, 1)

    @pl.when(core == 0)
    def _():
        for offset in OFFSETS:
            pl.semaphore_signal(barrier, inc=1, device_id=(ens, peer(offset) * 2 + 1), device_id_type=MESH)
        pl.semaphore_wait(barrier, 1)
        pl.semaphore_signal(hello, inc=1, device_id=(ens, partner), device_id_type=MESH)

    swaps = []
    for k, (load, src, dst) in enumerate((
        (loads[0], spare, theta.at[:, pl.ds(feat, feat)]), (loads[2], mean_own, mean_x),
        (loads[3], prec_own, prec_x), (loads[4], factor_own, factor_x),
    )):
        load.wait()
        copy = pltpu.make_async_remote_copy(src, dst, swap_send.at[k], swap_recv.at[k], device_id=(ens, partner), device_id_type=MESH)
        copy.start()
        swaps.append(copy)
    loads[1].wait()

    row_id = lax.broadcasted_iota(jnp.int32, (HALF, HALF), 0)
    col_id = lax.broadcasted_iota(jnp.int32, (HALF, HALF), 1)
    eye, upper = row_id == col_id, row_id <= col_id

    zeros = jnp.zeros((HALF - rank, 2 * feat), bf16)
    u_lo[rank:, :] = zeros
    u_hi[:HALF - rank, :] = zeros
    for copy in swaps:
        copy.wait_recv()
    factor = jnp.concatenate([factor_own[...], factor_x[...]], axis=1)
    u_lo[:rank, :] = factor
    u_hi[HALF - rank:, :] = factor
    mean_row = jnp.concatenate([mean_own[pl.ds(core, 1), :], mean_x[pl.ds(core, 1), :]], axis=1)
    prec_row = jnp.concatenate([prec_own[...], prec_x[...]], axis=1)
    others = pl.ds(0, CHIPS - 1)

    def drain(ref, sem):
        pltpu.make_async_copy(ref, ref, sem).wait()

    def partials():
        th = theta[...]
        tb = th.astype(bf16)
        xb = (th - mean_row).astype(bf16)
        top = lax.dot_general(tb[:HALF], tb, NT, preferred_element_type=f32)
        low = lax.dot_general(tb[HALF:], tb[HALF:], NT, preferred_element_type=f32)
        proj = (lax.dot_general(xb[:HALF], u_lo[...], NT, preferred_element_type=f32)
                + lax.dot_general(xb[HALF:], u_hi[...], NT, preferred_element_type=f32))
        tri = jnp.where(upper, top[:, :HALF], low)
        cross = top[:, HALF:]
        diag = jnp.sum(jnp.where(eye, low, 0.0), axis=0, keepdims=True)
        for o in range(CHIPS):
            block, r = (cross, 4 * o) if o < CHIPS // 2 else (tri, 4 * o - HALF)
            rs_send[o, 0:4, :] = block[r:r + 4]
            rs_send[o, 4:6, :] = proj[2 * o:2 * o + 2]
        diag_send[...] = diag

    def to_core(src, dst, ssem, rsem, target, on):
        return pltpu.make_async_remote_copy(src, dst, ssem, rsem, device_id=(ens, target * 2 + on), device_id_type=MESH)

    other = 1 - core

    def scatter():
        to_core(diag_send, diag_recv.at[chip], dr_ssem, dr_rsem, DIAG_CHIP, other).start()
        for offset in OFFSETS:
            target = peer(offset)
            to_core(rs_send.at[target], rs_recv.at[chip], rs_ssem, rs_rsem, target, other).start()

    def reduce():
        drain(rs_recv, rs_rsem)
        sums = [rs_recv[o] for o in range(4)]
        for o in range(4, CHIPS):
            sums[o % 4] = sums[o % 4] + rs_recv[o]
        total[...] = (sums[0] + sums[1]) + (sums[2] + sums[3])

    def reduce_diag():
        drain(diag_recv, dr_rsem)
        sums = [diag_recv[o] for o in range(4)]
        for o in range(4, CHIPS):
            sums[o % 4] = sums[o % 4] + diag_recv[o]
        diag_total[...] = (sums[0] + sums[1]) + (sums[2] + sums[3])

    def all_gather(last):
        @pl.when(chip == DIAG_CHIP)
        def _():
            reduce_diag()
            if last:
                for target in EARLY:
                    to_core(diag_total, diag_all.at[1], dg_ssem, dg_rsem.at[1], target, core).start()
            for offset in OFFSETS:
                to_core(diag_total, diag_all.at[0], dg_ssem, dg_rsem.at[0], peer(offset), other).start()

        if last:
            for target in EARLY:
                @pl.when(chip != target)
                def _():
                    to_core(total, gather.at[1, chip], ax_ssem, ag_rsem.at[1], target, core).start()
        for offset in OFFSETS:
            to_core(total, gather.at[0, chip], ag_ssem, ag_rsem.at[0], peer(offset), other).start()
        drain(rs_send, rs_ssem)
        drain(diag_send, dr_ssem)

    def sent(last):
        drain(gather.at[0], ag_ssem)

        @pl.when(chip == DIAG_CHIP)
        def _():
            drain(diag_recv, dg_ssem)
            if last:
                drain(diag_recv.at[pl.ds(0, len(EARLY))], dg_ssem)

        if last:
            drain(gather.at[1, pl.ds(0, len(EARLY) - 1)], ax_ssem) if len(EARLY) > 1 else None

            @pl.when(jnp.logical_not(early))
            def _():
                drain(total, ax_ssem)

    def kernel_matrix(k):
        diag = diag_all[k]
        cross = jnp.concatenate([gather[k, o, 0:4, :] for o in range(CHIPS // 2)], axis=0)
        tri = jnp.concatenate([gather[k, o, 0:4, :] for o in range(CHIPS // 2, CHIPS)], axis=0)
        proj = jnp.concatenate([gather[k, o, 4:6, :] for o in range(CHIPS)], axis=0).astype(bf16)
        tri_t, cross_t = tri.T, cross.T
        g_aa = jnp.where(upper, tri, tri_t)
        g_cc = jnp.where(eye, diag, jnp.where(upper, tri_t, tri))
        row_a = jnp.sum(jnp.where(eye, tri, 0.0), axis=0, keepdims=True)
        col_a = jnp.sum(jnp.where(eye, tri, 0.0), axis=1, keepdims=True)
        col_c = jnp.sum(jnp.where(eye, diag, 0.0), axis=1, keepdims=True)
        top = jnp.concatenate([g_aa, cross], axis=1)
        bottom = jnp.concatenate([cross_t, g_cc], axis=1)
        row_all = jnp.concatenate([row_a, diag], axis=1)
        k_top = jnp.exp(-jnp.maximum(col_a + row_all - 2.0 * top, 0.0) * inv_h)
        k_bot = jnp.exp(-jnp.maximum(col_c + row_all - 2.0 * bottom, 0.0) * inv_h)
        kernel = jnp.concatenate([k_top, k_bot], axis=0)
        keep = 1.0 + (scale * two_over_h) * jnp.sum(kernel, axis=1, keepdims=True)
        return kernel.astype(bf16), keep, proj

    def mixed(proj, still, cols):
        low = jnp.concatenate([
            jnp.dot(proj, u_lo[:, cols], preferred_element_type=f32),
            jnp.dot(proj, u_hi[:, cols], preferred_element_type=f32)], axis=0)
        return (still - low).astype(bf16)

    def moved(kernel_bf, keep, proj, th, still, cols):
        return keep * th + scale * jnp.dot(kernel_bf, mixed(proj, still, cols), preferred_element_type=f32)

    own = slice(0, feat)
    early = functools.reduce(jnp.logical_or, [chip == target for target in EARLY])
    partials()
    for copy in swaps:
        copy.wait_send()

    @pl.when(core == 1)
    def _():
        pl.semaphore_wait(barrier, 2 * CHIPS - 1)
        pl.semaphore_signal(go, inc=1, device_id=(ens, partner), device_id_type=MESH)

    @pl.when(core == 0)
    def _():
        pl.semaphore_wait(go, 1)

    @pl.when(core == 0)
    def _():
        pl.delay(LAG)

    scatter()

    @pl.loop(0, NUM_STEPS - 1)
    def _(_):
        base[...] = -((theta[...] - mean_row) * prec_row) - two_over_h * theta[...]
        reduce()
        all_gather(False)
        drain(diag_all.at[0], dg_rsem.at[0])
        drain(gather.at[0], ag_rsem.at[0])
        weights = kernel_matrix(0)
        for part in range(2):
            cols = slice(part * feat, (part + 1) * feat)
            theta[:, cols] = moved(*weights, theta[:, cols], base[:, cols], cols)
        partials()
        scatter()
        sent(False)

    def still(th, mean, prec):
        return -((th - mean) * prec) - two_over_h * th

    def back_copy(src, dst):
        return pltpu.make_async_remote_copy(src, dst, back_send, back_recv, device_id=(ens, partner), device_id_type=MESH)

    @pl.when(early)
    def _():
        back = back_copy(theta.at[:, pl.ds(feat, feat)], spare)
        back.start()
        base[:, own] = still(theta[:, own], mean_own[pl.ds(core, 1), :], prec_own[...])
        back.wait()
        base[:, feat:] = still(spare[...], mean_own[pl.ds(other, 1), :], prec_own[...])

    @pl.when(jnp.logical_not(early))
    def _():
        base[...] = still(theta[...], mean_row, prec_row)

    reduce()
    all_gather(True)
    drain(diag_all.at[0], dg_rsem.at[0])
    drain(gather.at[0], ag_rsem.at[0])

    @pl.when(early)
    def _():
        out_ref[core] = moved(*kernel_matrix(0), theta[:, own], base[:, own], own)
        gather[1, chip] = total[...]
        drain(diag_all.at[1], dg_rsem.at[1])
        drain(gather.at[1, others], ag_rsem.at[1])
        out_ref[other] = moved(*kernel_matrix(1), spare[...], base[:, feat:], own)

    @pl.when(jnp.logical_not(early))
    def _():
        weights = kernel_matrix(0)
        kernel_bf, keep, proj = weights
        partners = mixed(proj, base[:, feat:], slice(feat, 2 * feat))
        step = num_part // 2
        for r in range(0, num_part, step):
            rows = slice(r, r + step)
            spare[rows] = keep[rows] * theta[rows, feat:] + scale * jnp.dot(kernel_bf[rows], partners, preferred_element_type=f32)
            back_copy(spare.at[pl.ds(r, step)], out_ref.at[core, pl.ds(r, step)]).start()
        out_ref[core] = moved(*weights, theta[:, own], base[:, own], own)
        back_copy(spare, out_ref.at[other]).wait()

    sent(True)


def solution(mesh):
    feat_count = mesh.shape["feat"]
    data_spec = P("ens", None, "feat")
    mean_spec = P("ens", "feat")
    prec_spec = P(("ens", "feat"))
    factor_spec = P(("ens", "feat"), None)

    def local_steps(particles, target_mean, precision, low_factor):
        _, num_part, feat = particles.shape
        rank = low_factor.shape[1]
        total_feat = feat * feat_count
        bandwidth = 2.0 * total_feat
        consts = (2.0 / bandwidth, 1.0 / bandwidth, 0.25 * total_feat / num_part)
        hbm, vmem = pl.BlockSpec(memory_space=pl.ANY), pl.BlockSpec(memory_space=pltpu.VMEM)
        dma, regular = pltpu.SemaphoreType.DMA, pltpu.SemaphoreType.REGULAR
        f32, bf16 = jnp.float32, jnp.bfloat16
        return pl.pallas_call(
            functools.partial(_kernel, consts),
            name="svgd",
            out_shape=pltpu.VMEM(particles.shape, f32),
            in_specs=[hbm, hbm, hbm, hbm],
            out_specs=vmem,
            scratch_shapes=[
                pltpu.VMEM((num_part, 2 * feat), f32),
                pltpu.VMEM((num_part, 2 * feat), f32),
                pltpu.VMEM((num_part, feat), f32),
                pltpu.VMEM((2, feat), f32),
                pltpu.VMEM((2, feat), f32),
                pltpu.VMEM((1, feat), f32),
                pltpu.VMEM((1, feat), f32),
                pltpu.VMEM((rank, feat), bf16),
                pltpu.VMEM((rank, feat), bf16),
                pltpu.VMEM((CHIPS, 6, HALF), f32),
                pltpu.VMEM((CHIPS, 6, HALF), f32),
                pltpu.VMEM((6, HALF), f32),
                pltpu.VMEM((2, CHIPS, 6, HALF), f32),
                pltpu.VMEM((1, HALF), f32),
                pltpu.VMEM((CHIPS, 1, HALF), f32),
                pltpu.VMEM((1, HALF), f32),
                pltpu.VMEM((2, 1, HALF), f32),
                pltpu.VMEM((HALF, 2 * feat), bf16),
                pltpu.VMEM((HALF, 2 * feat), bf16),
                dma((5,)), dma((4,)), dma((4,)), regular, regular, dma, dma, dma, dma((2,)), dma, dma, dma, dma((2,)), dma, dma, dma,
            ],
            compiler_params=pltpu.CompilerParams(collective_id=0, has_side_effects=True),
        )(particles, target_mean, precision.reshape(1, feat), low_factor.T)

    return jax.shard_map(local_steps, mesh=mesh, in_specs=(data_spec, mean_spec, prec_spec, factor_spec), out_specs=data_spec, check_vma=False)
```

```python
import functools

import jax
import jax.numpy as jnp
from jax import lax
from jax.experimental import pallas as pl
from jax.experimental.pallas import tpu as pltpu
from jax.sharding import PartitionSpec as P

NUM_STEPS = 3
SIDE = 4
CHIPS = SIDE ** 3
HALF = 128
DIAG_CHIP = 21
EARLY = (0,)
LAG = 600
MESH = pl.DeviceIdType.MESH
NT = (((1,), (1,)), ((), ()))


COST = (0, 7, 10, 7)
OFFSETS = sorted(
    [(a, b, c) for a in range(SIDE) for b in range(SIDE) for c in range(SIDE)],
    key=lambda offset: -sum(COST[d] for d in offset),
)


def _kernel(consts, part_ref, mean_ref, prec_ref, factor_ref, out_ref,
            theta, base, spare, mean_own, mean_x, prec_own, prec_x, factor_own, factor_x, rs_send, rs_recv, total, gather, diag_send, diag_recv, diag_total, diag_all, u_two,
            load_sem, swap_send, swap_recv, hello, go, rs_ssem, rs_rsem, ag_ssem, ag_rsem, dr_ssem, dr_rsem, dg_ssem, dg_rsem, ax_ssem, back_send, back_recv):
    two_over_h, inv_h, scale = consts
    rank, feat = factor_ref.shape
    num_part = part_ref.shape[1]
    f32, bf16 = jnp.float32, jnp.bfloat16
    ens = lax.axis_index("ens")
    me = lax.axis_index("feat")
    core = me % 2
    chip = me // 2
    px, py, pz = chip % SIDE, (chip // SIDE) % SIDE, chip // (SIDE * SIDE)
    partner = chip * 2 + (1 - core)

    def peer(offset):
        dz, dy, dx = offset
        tz, ty, tx = (pz + dz) % SIDE, (py + dy) % SIDE, (px + dx) % SIDE
        return (tz * SIDE + ty) * SIDE + tx

    barrier = pltpu.get_barrier_semaphore()

    loads = []
    for k, (src, dst) in enumerate((
        (part_ref.at[1 - core], spare), (part_ref.at[core], theta.at[:, pl.ds(0, feat)]),
        (mean_ref, mean_own), (prec_ref, prec_own), (factor_ref, factor_own),
    )):
        copy = pltpu.make_async_copy(src, dst, load_sem.at[k])
        copy.start()
        loads.append(copy)

    @pl.when(core == 1)
    def _():
        pl.semaphore_signal(barrier, inc=1, device_id=(ens, partner), device_id_type=MESH)
        for offset in OFFSETS[:-1]:
            pl.semaphore_signal(barrier, inc=1, device_id=(ens, peer(offset) * 2 + 1), device_id_type=MESH)
        pl.semaphore_wait(hello, 1)

    @pl.when(core == 0)
    def _():
        for offset in OFFSETS:
            pl.semaphore_signal(barrier, inc=1, device_id=(ens, peer(offset) * 2 + 1), device_id_type=MESH)
        pl.semaphore_wait(barrier, 1)
        pl.semaphore_signal(hello, inc=1, device_id=(ens, partner), device_id_type=MESH)

    swaps = []
    for k, (load, src, dst) in enumerate((
        (loads[0], spare, theta.at[:, pl.ds(feat, feat)]), (loads[2], mean_own, mean_x),
        (loads[3], prec_own, prec_x), (loads[4], factor_own, factor_x),
    )):
        load.wait()
        copy = pltpu.make_async_remote_copy(src, dst, swap_send.at[k], swap_recv.at[k], device_id=(ens, partner), device_id_type=MESH)
        copy.start()
        swaps.append(copy)
    loads[1].wait()

    row_id = lax.broadcasted_iota(jnp.int32, (HALF, HALF), 0)
    col_id = lax.broadcasted_iota(jnp.int32, (HALF, HALF), 1)
    eye, upper = row_id == col_id, row_id <= col_id

    for copy in swaps:
        copy.wait_recv()
    factor = jnp.concatenate([factor_own[...], factor_x[...]], axis=1)
    u_two[:rank, :] = factor
    u_two[rank:, :] = factor
    mean_row = jnp.concatenate([mean_own[pl.ds(core, 1), :], mean_x[pl.ds(core, 1), :]], axis=1)
    prec_row = jnp.concatenate([prec_own[...], prec_x[...]], axis=1)
    others = pl.ds(0, CHIPS - 1)

    def drain(ref, sem):
        pltpu.make_async_copy(ref, ref, sem).wait()

    def partials():
        th = theta[...]
        tb = th.astype(bf16)
        xb = (th - mean_row).astype(bf16)
        gram = lax.dot_general(tb, tb, NT, preferred_element_type=f32)
        twice = lax.dot_general(xb, u_two[...], NT, preferred_element_type=f32)
        proj = jnp.where(col_id < rank, twice[:HALF], twice[HALF:])
        cross, low = gram[:HALF, HALF:], gram[HALF:, HALF:]
        tri = jnp.where(upper, gram[:HALF, :HALF], low)
        diag = jnp.sum(jnp.where(eye, low, 0.0), axis=0, keepdims=True)
        for o in range(CHIPS):
            block, r = (cross, 4 * o) if o < CHIPS // 2 else (tri, 4 * o - HALF)
            rs_send[o, 0:4, :] = block[r:r + 4]
            rs_send[o, 4:6, :] = proj[2 * o:2 * o + 2]
        diag_send[...] = diag

    def to_core(src, dst, ssem, rsem, target, on):
        return pltpu.make_async_remote_copy(src, dst, ssem, rsem, device_id=(ens, target * 2 + on), device_id_type=MESH)

    other = 1 - core

    def scatter():
        to_core(diag_send, diag_recv.at[chip], dr_ssem, dr_rsem, DIAG_CHIP, other).start()
        for offset in OFFSETS:
            target = peer(offset)
            to_core(rs_send.at[target], rs_recv.at[chip], rs_ssem, rs_rsem, target, other).start()

    def reduce():
        drain(rs_recv, rs_rsem)
        sums = [rs_recv[o] for o in range(4)]
        for o in range(4, CHIPS):
            sums[o % 4] = sums[o % 4] + rs_recv[o]
        total[...] = (sums[0] + sums[1]) + (sums[2] + sums[3])

    def reduce_diag():
        drain(diag_recv, dr_rsem)
        sums = [diag_recv[o] for o in range(4)]
        for o in range(4, CHIPS):
            sums[o % 4] = sums[o % 4] + diag_recv[o]
        diag_total[...] = (sums[0] + sums[1]) + (sums[2] + sums[3])

    def all_gather(last):
        @pl.when(chip == DIAG_CHIP)
        def _():
            reduce_diag()
            if last:
                for target in EARLY:
                    to_core(diag_total, diag_all.at[1], dg_ssem, dg_rsem.at[1], target, core).start()
            for offset in OFFSETS:
                to_core(diag_total, diag_all.at[0], dg_ssem, dg_rsem.at[0], peer(offset), other).start()

        if last:
            for target in EARLY:
                @pl.when(chip != target)
                def _():
                    to_core(total, gather.at[1, chip], ax_ssem, ag_rsem.at[1], target, core).start()
        for offset in OFFSETS:
            to_core(total, gather.at[0, chip], ag_ssem, ag_rsem.at[0], peer(offset), other).start()
        drain(rs_send, rs_ssem)
        drain(diag_send, dr_ssem)

    def sent(last):
        drain(gather.at[0], ag_ssem)

        @pl.when(chip == DIAG_CHIP)
        def _():
            drain(diag_recv, dg_ssem)
            if last:
                drain(diag_recv.at[pl.ds(0, len(EARLY))], dg_ssem)

        if last:
            drain(gather.at[1, pl.ds(0, len(EARLY) - 1)], ax_ssem) if len(EARLY) > 1 else None

            @pl.when(jnp.logical_not(early))
            def _():
                drain(total, ax_ssem)

    def kernel_matrix(k):
        diag = diag_all[k]
        cross = jnp.concatenate([gather[k, o, 0:4, :] for o in range(CHIPS // 2)], axis=0)
        tri = jnp.concatenate([gather[k, o, 0:4, :] for o in range(CHIPS // 2, CHIPS)], axis=0)
        proj = jnp.concatenate([gather[k, o, 4:6, :] for o in range(CHIPS)], axis=0)
        proj = jnp.concatenate([jnp.where(col_id < rank, proj, 0.0), jnp.where(col_id < rank, 0.0, proj)], axis=0).astype(bf16)
        tri_t, cross_t = tri.T, cross.T
        g_aa = jnp.where(upper, tri, tri_t)
        g_cc = jnp.where(eye, diag, jnp.where(upper, tri_t, tri))
        row_a = jnp.sum(jnp.where(eye, tri, 0.0), axis=0, keepdims=True)
        col_a = jnp.sum(jnp.where(eye, tri, 0.0), axis=1, keepdims=True)
        col_c = jnp.sum(jnp.where(eye, diag, 0.0), axis=1, keepdims=True)
        top = jnp.concatenate([g_aa, cross], axis=1)
        bottom = jnp.concatenate([cross_t, g_cc], axis=1)
        row_all = jnp.concatenate([row_a, diag], axis=1)
        k_top = jnp.exp(-jnp.maximum(col_a + row_all - 2.0 * top, 0.0) * inv_h)
        k_bot = jnp.exp(-jnp.maximum(col_c + row_all - 2.0 * bottom, 0.0) * inv_h)
        kernel = jnp.concatenate([k_top, k_bot], axis=0)
        keep = 1.0 + (scale * two_over_h) * jnp.sum(kernel, axis=1, keepdims=True)
        return kernel.astype(bf16), keep, proj

    def mixed(proj, still, cols):
        return (still - jnp.dot(proj, u_two[:, cols], preferred_element_type=f32)).astype(bf16)

    def moved(kernel_bf, keep, proj, th, still, cols):
        return keep * th + scale * jnp.dot(kernel_bf, mixed(proj, still, cols), preferred_element_type=f32)

    own = slice(0, feat)
    early = functools.reduce(jnp.logical_or, [chip == target for target in EARLY])
    partials()
    for copy in swaps:
        copy.wait_send()

    @pl.when(core == 1)
    def _():
        pl.semaphore_wait(barrier, 2 * CHIPS - 1)
        pl.semaphore_signal(go, inc=1, device_id=(ens, partner), device_id_type=MESH)

    @pl.when(core == 0)
    def _():
        pl.semaphore_wait(go, 1)

    @pl.when(core == 0)
    def _():
        pl.delay(LAG)

    scatter()

    @pl.loop(0, NUM_STEPS - 1)
    def _(_):
        base[...] = -((theta[...] - mean_row) * prec_row) - two_over_h * theta[...]
        reduce()
        all_gather(False)
        drain(diag_all.at[0], dg_rsem.at[0])
        drain(gather.at[0], ag_rsem.at[0])
        weights = kernel_matrix(0)
        theta[...] = moved(*weights, theta[...], base[...], slice(0, 2 * feat))
        partials()
        scatter()
        sent(False)

    def still(th, mean, prec):
        return -((th - mean) * prec) - two_over_h * th

    def back_copy(src, dst):
        return pltpu.make_async_remote_copy(src, dst, back_send, back_recv, device_id=(ens, partner), device_id_type=MESH)

    @pl.when(early)
    def _():
        back = back_copy(theta.at[:, pl.ds(feat, feat)], spare)
        back.start()
        base[:, own] = still(theta[:, own], mean_own[pl.ds(core, 1), :], prec_own[...])
        back.wait()
        base[:, feat:] = still(spare[...], mean_own[pl.ds(other, 1), :], prec_own[...])

    @pl.when(jnp.logical_not(early))
    def _():
        base[...] = still(theta[...], mean_row, prec_row)

    reduce()
    all_gather(True)
    drain(diag_all.at[0], dg_rsem.at[0])
    drain(gather.at[0], ag_rsem.at[0])

    @pl.when(early)
    def _():
        out_ref[core] = moved(*kernel_matrix(0), theta[:, own], base[:, own], own)
        gather[1, chip] = total[...]
        drain(diag_all.at[1], dg_rsem.at[1])
        drain(gather.at[1, others], ag_rsem.at[1])
        out_ref[other] = moved(*kernel_matrix(1), spare[...], base[:, feat:], own)

    @pl.when(jnp.logical_not(early))
    def _():
        weights = kernel_matrix(0)
        kernel_bf, keep, proj = weights
        partners = mixed(proj, base[:, feat:], slice(feat, 2 * feat))
        step = num_part // 2
        for r in range(0, num_part, step):
            rows = slice(r, r + step)
            spare[rows] = keep[rows] * theta[rows, feat:] + scale * jnp.dot(kernel_bf[rows], partners, preferred_element_type=f32)
            back_copy(spare.at[pl.ds(r, step)], out_ref.at[core, pl.ds(r, step)]).start()
        out_ref[core] = moved(*weights, theta[:, own], base[:, own], own)
        back_copy(spare, out_ref.at[other]).wait()

    sent(True)


def solution(mesh):
    feat_count = mesh.shape["feat"]
    data_spec = P("ens", None, "feat")
    mean_spec = P("ens", "feat")
    prec_spec = P(("ens", "feat"))
    factor_spec = P(("ens", "feat"), None)

    def local_steps(particles, target_mean, precision, low_factor):
        _, num_part, feat = particles.shape
        rank = low_factor.shape[1]
        total_feat = feat * feat_count
        bandwidth = 2.0 * total_feat
        consts = (2.0 / bandwidth, 1.0 / bandwidth, 0.25 * total_feat / num_part)
        hbm, vmem = pl.BlockSpec(memory_space=pl.ANY), pl.BlockSpec(memory_space=pltpu.VMEM)
        dma, regular = pltpu.SemaphoreType.DMA, pltpu.SemaphoreType.REGULAR
        f32, bf16 = jnp.float32, jnp.bfloat16
        return pl.pallas_call(
            functools.partial(_kernel, consts),
            name="svgd",
            out_shape=pltpu.VMEM(particles.shape, f32),
            in_specs=[hbm, hbm, hbm, hbm],
            out_specs=vmem,
            scratch_shapes=[
                pltpu.VMEM((num_part, 2 * feat), f32),
                pltpu.VMEM((num_part, 2 * feat), f32),
                pltpu.VMEM((num_part, feat), f32),
                pltpu.VMEM((2, feat), f32),
                pltpu.VMEM((2, feat), f32),
                pltpu.VMEM((1, feat), f32),
                pltpu.VMEM((1, feat), f32),
                pltpu.VMEM((rank, feat), bf16),
                pltpu.VMEM((rank, feat), bf16),
                pltpu.VMEM((CHIPS, 6, HALF), f32),
                pltpu.VMEM((CHIPS, 6, HALF), f32),
                pltpu.VMEM((6, HALF), f32),
                pltpu.VMEM((2, CHIPS, 6, HALF), f32),
                pltpu.VMEM((1, HALF), f32),
                pltpu.VMEM((CHIPS, 1, HALF), f32),
                pltpu.VMEM((1, HALF), f32),
                pltpu.VMEM((2, 1, HALF), f32),
                pltpu.VMEM((2 * rank, 2 * feat), bf16),
                dma((5,)), dma((4,)), dma((4,)), regular, regular, dma, dma, dma, dma((2,)), dma, dma, dma, dma((2,)), dma, dma, dma,
            ],
            compiler_params=pltpu.CompilerParams(collective_id=0, has_side_effects=True),
        )(particles, target_mean, precision.reshape(1, feat), low_factor.T)

    return jax.shard_map(local_steps, mesh=mesh, in_specs=(data_spec, mean_spec, prec_spec, factor_spec), out_specs=data_spec, check_vma=False)
```

```python
import functools

import jax
import jax.numpy as jnp
from jax import lax
from jax.experimental import pallas as pl
from jax.experimental.pallas import tpu as pltpu
from jax.sharding import PartitionSpec as P

NUM_STEPS = 3
SIDE = 4
CHIPS = SIDE ** 3
HALF = 128
DIAG_CHIP = 20
EARLY = (0,)
LAG = 600
MESH = pl.DeviceIdType.MESH
NT = (((1,), (1,)), ((), ()))


COST = (0, 7, 10, 7)
OFFSETS = sorted(
    [(a, b, c) for a in range(SIDE) for b in range(SIDE) for c in range(SIDE)],
    key=lambda offset: -sum(COST[d] for d in offset),
)


def _kernel(consts, part_ref, mean_ref, prec_ref, factor_ref, out_ref,
            theta, base, spare, mean_own, mean_x, prec_own, prec_x, factor_own, factor_x, rs_send, rs_recv, total, gather, diag_send, diag_recv, diag_total, diag_all, u_two,
            load_sem, swap_send, swap_recv, hello, go, rs_ssem, rs_rsem, ag_ssem, ag_rsem, dr_ssem, dr_rsem, dg_ssem, dg_rsem, ax_ssem, back_send, back_recv):
    two_over_h, inv_h, scale = consts
    rank, feat = factor_ref.shape
    num_part = part_ref.shape[1]
    f32, bf16 = jnp.float32, jnp.bfloat16
    ens = lax.axis_index("ens")
    me = lax.axis_index("feat")
    core = me % 2
    chip = me // 2
    px, py, pz = chip % SIDE, (chip // SIDE) % SIDE, chip // (SIDE * SIDE)
    partner = chip * 2 + (1 - core)

    def peer(offset):
        dz, dy, dx = offset
        tz, ty, tx = (pz + dz) % SIDE, (py + dy) % SIDE, (px + dx) % SIDE
        return (tz * SIDE + ty) * SIDE + tx

    barrier = pltpu.get_barrier_semaphore()

    loads = []
    for k, (src, dst) in enumerate((
        (part_ref.at[1 - core], spare), (part_ref.at[core], theta.at[:, pl.ds(0, feat)]),
        (mean_ref, mean_own), (prec_ref, prec_own), (factor_ref, factor_own),
    )):
        copy = pltpu.make_async_copy(src, dst, load_sem.at[k])
        copy.start()
        loads.append(copy)

    @pl.when(core == 1)
    def _():
        pl.semaphore_signal(barrier, inc=1, device_id=(ens, partner), device_id_type=MESH)
        for offset in OFFSETS[:-1]:
            pl.semaphore_signal(barrier, inc=1, device_id=(ens, peer(offset) * 2 + 1), device_id_type=MESH)
        pl.semaphore_wait(hello, 1)

    @pl.when(core == 0)
    def _():
        for offset in OFFSETS:
            pl.semaphore_signal(barrier, inc=1, device_id=(ens, peer(offset) * 2 + 1), device_id_type=MESH)
        pl.semaphore_wait(barrier, 1)
        pl.semaphore_signal(hello, inc=1, device_id=(ens, partner), device_id_type=MESH)

    swaps = []
    for k, (load, src, dst) in enumerate((
        (loads[0], spare, theta.at[:, pl.ds(feat, feat)]), (loads[2], mean_own, mean_x),
        (loads[3], prec_own, prec_x), (loads[4], factor_own, factor_x),
    )):
        load.wait()
        copy = pltpu.make_async_remote_copy(src, dst, swap_send.at[k], swap_recv.at[k], device_id=(ens, partner), device_id_type=MESH)
        copy.start()
        swaps.append(copy)
    loads[1].wait()

    row_id = lax.broadcasted_iota(jnp.int32, (HALF, HALF), 0)
    col_id = lax.broadcasted_iota(jnp.int32, (HALF, HALF), 1)
    eye, upper = row_id == col_id, row_id <= col_id

    for copy in swaps:
        copy.wait_recv()
    factor = jnp.concatenate([factor_own[...], factor_x[...]], axis=1)
    u_two[:rank, :] = factor
    u_two[rank:, :] = factor
    mean_row = jnp.concatenate([mean_own[pl.ds(core, 1), :], mean_x[pl.ds(core, 1), :]], axis=1)
    prec_row = jnp.concatenate([prec_own[...], prec_x[...]], axis=1)
    others = pl.ds(0, CHIPS - 1)

    def drain(ref, sem):
        pltpu.make_async_copy(ref, ref, sem).wait()

    def partials(th):
        tb = th.astype(bf16)
        xb = (th - mean_row).astype(bf16)
        gram = lax.dot_general(tb, tb, NT, preferred_element_type=f32)
        twice = lax.dot_general(xb, u_two[...], NT, preferred_element_type=f32)
        proj = jnp.where(col_id < rank, twice[:HALF], twice[HALF:])
        cross, low = gram[:HALF, HALF:], gram[HALF:, HALF:]
        tri = jnp.where(upper, gram[:HALF, :HALF], low)
        diag = jnp.sum(jnp.where(eye, low, 0.0), axis=0, keepdims=True)
        for o in range(CHIPS):
            block, r = (cross, 4 * o) if o < CHIPS // 2 else (tri, 4 * o - HALF)
            rs_send[o, 0:4, :] = block[r:r + 4]
            rs_send[o, 4:6, :] = proj[2 * o:2 * o + 2]
        diag_send[...] = diag

    def to_core(src, dst, ssem, rsem, target, on):
        return pltpu.make_async_remote_copy(src, dst, ssem, rsem, device_id=(ens, target * 2 + on), device_id_type=MESH)

    other = 1 - core

    def scatter():
        to_core(diag_send, diag_recv.at[chip], dr_ssem, dr_rsem, DIAG_CHIP, other).start()
        for offset in OFFSETS:
            target = peer(offset)
            to_core(rs_send.at[target], rs_recv.at[chip], rs_ssem, rs_rsem, target, other).start()

    def reduce():
        drain(rs_recv, rs_rsem)
        sums = [rs_recv[o] for o in range(4)]
        for o in range(4, CHIPS):
            sums[o % 4] = sums[o % 4] + rs_recv[o]
        total[...] = (sums[0] + sums[1]) + (sums[2] + sums[3])

    def reduce_diag():
        drain(diag_recv, dr_rsem)
        sums = [diag_recv[o] for o in range(4)]
        for o in range(4, CHIPS):
            sums[o % 4] = sums[o % 4] + diag_recv[o]
        diag_total[...] = (sums[0] + sums[1]) + (sums[2] + sums[3])

    def all_gather(last):
        @pl.when(chip == DIAG_CHIP)
        def _():
            reduce_diag()
            if last:
                for target in EARLY:
                    to_core(diag_total, diag_all.at[1], dg_ssem, dg_rsem.at[1], target, core).start()
            for offset in OFFSETS:
                to_core(diag_total, diag_all.at[0], dg_ssem, dg_rsem.at[0], peer(offset), other).start()

        if last:
            for target in EARLY:
                @pl.when(chip != target)
                def _():
                    to_core(total, gather.at[1, chip], ax_ssem, ag_rsem.at[1], target, core).start()
        for offset in OFFSETS:
            to_core(total, gather.at[0, chip], ag_ssem, ag_rsem.at[0], peer(offset), other).start()
        drain(rs_send, rs_ssem)
        drain(diag_send, dr_ssem)

    def sent(last):
        drain(gather.at[0], ag_ssem)

        @pl.when(chip == DIAG_CHIP)
        def _():
            drain(diag_recv, dg_ssem)
            if last:
                drain(diag_recv.at[pl.ds(0, len(EARLY))], dg_ssem)

        if last:
            drain(gather.at[1, pl.ds(0, len(EARLY) - 1)], ax_ssem) if len(EARLY) > 1 else None

            @pl.when(jnp.logical_not(early))
            def _():
                drain(total, ax_ssem)

    def kernel_matrix(k):
        diag = diag_all[k]
        cross = jnp.concatenate([gather[k, o, 0:4, :] for o in range(CHIPS // 2)], axis=0)
        tri = jnp.concatenate([gather[k, o, 0:4, :] for o in range(CHIPS // 2, CHIPS)], axis=0)
        proj = jnp.concatenate([gather[k, o, 4:6, :] for o in range(CHIPS)], axis=0)
        proj = jnp.concatenate([jnp.where(col_id < rank, proj, 0.0), jnp.where(col_id < rank, 0.0, proj)], axis=0).astype(bf16)
        tri_t, cross_t = tri.T, cross.T
        g_aa = jnp.where(upper, tri, tri_t)
        g_cc = jnp.where(eye, diag, jnp.where(upper, tri_t, tri))
        row_a = jnp.sum(jnp.where(eye, tri, 0.0), axis=0, keepdims=True)
        col_a = jnp.sum(jnp.where(eye, tri, 0.0), axis=1, keepdims=True)
        col_c = jnp.sum(jnp.where(eye, diag, 0.0), axis=1, keepdims=True)
        top = jnp.concatenate([g_aa, cross], axis=1)
        bottom = jnp.concatenate([cross_t, g_cc], axis=1)
        row_all = jnp.concatenate([row_a, diag], axis=1)
        k_top = jnp.exp(-jnp.maximum(col_a + row_all - 2.0 * top, 0.0) * inv_h)
        k_bot = jnp.exp(-jnp.maximum(col_c + row_all - 2.0 * bottom, 0.0) * inv_h)
        kernel = jnp.concatenate([k_top, k_bot], axis=0)
        keep = 1.0 + (scale * two_over_h) * jnp.sum(kernel, axis=1, keepdims=True)
        return kernel.astype(bf16), keep, proj

    def mixed(proj, still, cols):
        return (still - jnp.dot(proj, u_two[:, cols], preferred_element_type=f32)).astype(bf16)

    def moved(kernel_bf, keep, proj, th, still, cols):
        return keep * th + scale * jnp.dot(kernel_bf, mixed(proj, still, cols), preferred_element_type=f32)

    own = slice(0, feat)
    early = functools.reduce(jnp.logical_or, [chip == target for target in EARLY])
    partials(theta[...])
    for copy in swaps:
        copy.wait_send()

    @pl.when(core == 1)
    def _():
        pl.semaphore_wait(barrier, 2 * CHIPS - 1)
        pl.semaphore_signal(go, inc=1, device_id=(ens, partner), device_id_type=MESH)

    @pl.when(core == 0)
    def _():
        pl.semaphore_wait(go, 1)

    @pl.when(core == 0)
    def _():
        pl.delay(LAG)

    scatter()

    @pl.loop(0, NUM_STEPS - 1)
    def _(_):
        base[...] = -((theta[...] - mean_row) * prec_row) - two_over_h * theta[...]
        reduce()
        all_gather(False)
        drain(diag_all.at[0], dg_rsem.at[0])
        drain(gather.at[0], ag_rsem.at[0])
        weights = kernel_matrix(0)
        new = moved(*weights, theta[...], base[...], slice(0, 2 * feat))
        theta[...] = new
        partials(new)
        scatter()
        sent(False)

    def still(th, mean, prec):
        return -((th - mean) * prec) - two_over_h * th

    def back_copy(src, dst):
        return pltpu.make_async_remote_copy(src, dst, back_send, back_recv, device_id=(ens, partner), device_id_type=MESH)

    @pl.when(early)
    def _():
        back = back_copy(theta.at[:, pl.ds(feat, feat)], spare)
        back.start()
        base[:, own] = still(theta[:, own], mean_own[pl.ds(core, 1), :], prec_own[...])
        back.wait()
        base[:, feat:] = still(spare[...], mean_own[pl.ds(other, 1), :], prec_own[...])

    @pl.when(jnp.logical_not(early))
    def _():
        base[...] = still(theta[...], mean_row, prec_row)

    reduce()
    all_gather(True)
    drain(diag_all.at[0], dg_rsem.at[0])
    drain(gather.at[0], ag_rsem.at[0])

    @pl.when(early)
    def _():
        out_ref[core] = moved(*kernel_matrix(0), theta[:, own], base[:, own], own)
        gather[1, chip] = total[...]
        drain(diag_all.at[1], dg_rsem.at[1])
        drain(gather.at[1, others], ag_rsem.at[1])
        out_ref[other] = moved(*kernel_matrix(1), spare[...], base[:, feat:], own)

    @pl.when(jnp.logical_not(early))
    def _():
        weights = kernel_matrix(0)
        kernel_bf, keep, proj = weights
        partners = mixed(proj, base[:, feat:], slice(feat, 2 * feat))
        step = num_part // 2
        for r in range(0, num_part, step):
            rows = slice(r, r + step)
            spare[rows] = keep[rows] * theta[rows, feat:] + scale * jnp.dot(kernel_bf[rows], partners, preferred_element_type=f32)
            back_copy(spare.at[pl.ds(r, step)], out_ref.at[core, pl.ds(r, step)]).start()
        out_ref[core] = moved(*weights, theta[:, own], base[:, own], own)
        back_copy(spare, out_ref.at[other]).wait()

    sent(True)


def solution(mesh):
    feat_count = mesh.shape["feat"]
    data_spec = P("ens", None, "feat")
    mean_spec = P("ens", "feat")
    prec_spec = P(("ens", "feat"))
    factor_spec = P(("ens", "feat"), None)

    def local_steps(particles, target_mean, precision, low_factor):
        _, num_part, feat = particles.shape
        rank = low_factor.shape[1]
        total_feat = feat * feat_count
        bandwidth = 2.0 * total_feat
        consts = (2.0 / bandwidth, 1.0 / bandwidth, 0.25 * total_feat / num_part)
        hbm, vmem = pl.BlockSpec(memory_space=pl.ANY), pl.BlockSpec(memory_space=pltpu.VMEM)
        dma, regular = pltpu.SemaphoreType.DMA, pltpu.SemaphoreType.REGULAR
        f32, bf16 = jnp.float32, jnp.bfloat16
        return pl.pallas_call(
            functools.partial(_kernel, consts),
            name="svgd",
            out_shape=pltpu.VMEM(particles.shape, f32),
            in_specs=[hbm, hbm, hbm, hbm],
            out_specs=vmem,
            scratch_shapes=[
                pltpu.VMEM((num_part, 2 * feat), f32),
                pltpu.VMEM((num_part, 2 * feat), f32),
                pltpu.VMEM((num_part, feat), f32),
                pltpu.VMEM((2, feat), f32),
                pltpu.VMEM((2, feat), f32),
                pltpu.VMEM((1, feat), f32),
                pltpu.VMEM((1, feat), f32),
                pltpu.VMEM((rank, feat), bf16),
                pltpu.VMEM((rank, feat), bf16),
                pltpu.VMEM((CHIPS, 6, HALF), f32),
                pltpu.VMEM((CHIPS, 6, HALF), f32),
                pltpu.VMEM((6, HALF), f32),
                pltpu.VMEM((2, CHIPS, 6, HALF), f32),
                pltpu.VMEM((1, HALF), f32),
                pltpu.VMEM((CHIPS, 1, HALF), f32),
                pltpu.VMEM((1, HALF), f32),
                pltpu.VMEM((2, 1, HALF), f32),
                pltpu.VMEM((2 * rank, 2 * feat), bf16),
                dma((5,)), dma((4,)), dma((4,)), regular, regular, dma, dma, dma, dma((2,)), dma, dma, dma, dma((2,)), dma, dma, dma,
            ],
            compiler_params=pltpu.CompilerParams(collective_id=0, has_side_effects=True),
        )(particles, target_mean, precision.reshape(1, feat), low_factor.T)

    return jax.shard_map(local_steps, mesh=mesh, in_specs=(data_spec, mean_spec, prec_spec, factor_spec), out_specs=data_spec, check_vma=False)
```

```python
import functools

import jax
import jax.numpy as jnp
from jax import lax
from jax.experimental import pallas as pl
from jax.experimental.pallas import tpu as pltpu
from jax.sharding import PartitionSpec as P

NUM_STEPS = 3
SIDE = 4
CHIPS = SIDE ** 3
HALF = 128
DIAG_CHIP = 20
EARLY = (0,)
LAG = 600
MESH = pl.DeviceIdType.MESH
NT = (((1,), (1,)), ((), ()))


COST = (0, 7, 10, 7)
OFFSETS = sorted(
    [(a, b, c) for a in range(SIDE) for b in range(SIDE) for c in range(SIDE)],
    key=lambda offset: -sum(COST[d] for d in offset),
)


def _kernel(consts, part_ref, mean_ref, prec_ref, factor_ref, out_ref,
            theta, base, spare, mean_own, mean_x, prec_own, prec_x, factor_own, factor_x, rs_send, rs_recv, total, gather, diag_send, diag_recv, diag_total, diag_all, u_two,
            load_sem, swap_send, swap_recv, hello, go, rs_ssem, rs_rsem, ag_ssem, ag_rsem, dr_ssem, dr_rsem, dg_ssem, dg_rsem, ax_ssem, back_send, back_recv):
    two_over_h, inv_h, scale = consts
    rank, feat = factor_ref.shape
    num_part = part_ref.shape[1]
    f32, bf16 = jnp.float32, jnp.bfloat16
    ens = lax.axis_index("ens")
    me = lax.axis_index("feat")
    core = me % 2
    chip = me // 2
    px, py, pz = chip % SIDE, (chip // SIDE) % SIDE, chip // (SIDE * SIDE)
    partner = chip * 2 + (1 - core)

    def peer(offset):
        dz, dy, dx = offset
        tz, ty, tx = (pz + dz) % SIDE, (py + dy) % SIDE, (px + dx) % SIDE
        return (tz * SIDE + ty) * SIDE + tx

    barrier = pltpu.get_barrier_semaphore()

    loads = []
    for k, (src, dst) in enumerate((
        (part_ref.at[1 - core], spare), (part_ref.at[core], theta.at[:, pl.ds(0, feat)]),
        (mean_ref, mean_own), (prec_ref, prec_own), (factor_ref, factor_own),
    )):
        copy = pltpu.make_async_copy(src, dst, load_sem.at[k])
        copy.start()
        loads.append(copy)

    @pl.when(core == 1)
    def _():
        pl.semaphore_signal(barrier, inc=1, device_id=(ens, partner), device_id_type=MESH)
        for offset in OFFSETS[:-1]:
            pl.semaphore_signal(barrier, inc=1, device_id=(ens, peer(offset) * 2 + 1), device_id_type=MESH)
        pl.semaphore_wait(hello, 1)

    @pl.when(core == 0)
    def _():
        for offset in OFFSETS:
            pl.semaphore_signal(barrier, inc=1, device_id=(ens, peer(offset) * 2 + 1), device_id_type=MESH)
        pl.semaphore_wait(barrier, 1)
        pl.semaphore_signal(hello, inc=1, device_id=(ens, partner), device_id_type=MESH)

    swaps = []
    for k, (load, src, dst) in enumerate((
        (loads[0], spare, theta.at[:, pl.ds(feat, feat)]), (loads[2], mean_own, mean_x),
        (loads[3], prec_own, prec_x), (loads[4], factor_own, factor_x),
    )):
        load.wait()
        copy = pltpu.make_async_remote_copy(src, dst, swap_send.at[k], swap_recv.at[k], device_id=(ens, partner), device_id_type=MESH)
        copy.start()
        swaps.append(copy)
    loads[1].wait()

    row_id = lax.broadcasted_iota(jnp.int32, (HALF, HALF), 0)
    col_id = lax.broadcasted_iota(jnp.int32, (HALF, HALF), 1)
    eye, upper = row_id == col_id, row_id <= col_id

    for copy in swaps:
        copy.wait_recv()
    factor = jnp.concatenate([factor_own[...], factor_x[...]], axis=1)
    u_two[:rank, :] = factor
    u_two[rank:, :] = factor
    mean_row = jnp.concatenate([mean_own[pl.ds(core, 1), :], mean_x[pl.ds(core, 1), :]], axis=1)
    prec_row = jnp.concatenate([prec_own[...], prec_x[...]], axis=1)
    others = pl.ds(0, CHIPS - 1)

    def drain(ref, sem):
        pltpu.make_async_copy(ref, ref, sem).wait()

    def partials(th):
        tb = th.astype(bf16)
        xb = (th - mean_row).astype(bf16)
        gram = lax.dot_general(tb, tb, NT, preferred_element_type=f32)
        twice = lax.dot_general(xb, u_two[...], NT, preferred_element_type=f32)
        proj = jnp.where(col_id < rank, twice[:HALF], twice[HALF:])
        cross, low = gram[:HALF, HALF:], gram[HALF:, HALF:]
        tri = jnp.where(upper, gram[:HALF, :HALF], low)
        diag = jnp.sum(jnp.where(eye, low, 0.0), axis=0, keepdims=True)
        for o in range(CHIPS):
            block, r = (cross, 4 * o) if o < CHIPS // 2 else (tri, 4 * o - HALF)
            rs_send[o, 0:4, :] = block[r:r + 4]
            rs_send[o, 4:6, :] = proj[2 * o:2 * o + 2]
        diag_send[...] = diag

    def to_core(src, dst, ssem, rsem, target, on):
        return pltpu.make_async_remote_copy(src, dst, ssem, rsem, device_id=(ens, target * 2 + on), device_id_type=MESH)

    other = 1 - core

    def scatter():
        to_core(diag_send, diag_recv.at[chip], dr_ssem, dr_rsem, DIAG_CHIP, other).start()
        for offset in OFFSETS:
            target = peer(offset)
            to_core(rs_send.at[target], rs_recv.at[chip], rs_ssem, rs_rsem, target, other).start()

    def reduce():
        drain(rs_recv, rs_rsem)
        terms = [rs_recv[o] for o in range(CHIPS)]
        while len(terms) > 1:
            terms = [a + b for a, b in zip(terms[::2], terms[1::2])]
        total[...] = terms[0]

    def reduce_diag():
        drain(diag_recv, dr_rsem)
        sums = [diag_recv[o] for o in range(4)]
        for o in range(4, CHIPS):
            sums[o % 4] = sums[o % 4] + diag_recv[o]
        diag_total[...] = (sums[0] + sums[1]) + (sums[2] + sums[3])

    def all_gather(last):
        @pl.when(chip == DIAG_CHIP)
        def _():
            reduce_diag()
            if last:
                for target in EARLY:
                    to_core(diag_total, diag_all.at[1], dg_ssem, dg_rsem.at[1], target, core).start()
            for offset in OFFSETS:
                to_core(diag_total, diag_all.at[0], dg_ssem, dg_rsem.at[0], peer(offset), other).start()

        if last:
            for target in EARLY:
                @pl.when(chip != target)
                def _():
                    to_core(total, gather.at[1, chip], ax_ssem, ag_rsem.at[1], target, core).start()
        for offset in OFFSETS:
            to_core(total, gather.at[0, chip], ag_ssem, ag_rsem.at[0], peer(offset), other).start()
        drain(rs_send, rs_ssem)
        drain(diag_send, dr_ssem)

    def sent(last):
        drain(gather.at[0], ag_ssem)

        @pl.when(chip == DIAG_CHIP)
        def _():
            drain(diag_recv, dg_ssem)
            if last:
                drain(diag_recv.at[pl.ds(0, len(EARLY))], dg_ssem)

        if last:
            drain(gather.at[1, pl.ds(0, len(EARLY) - 1)], ax_ssem) if len(EARLY) > 1 else None

            @pl.when(jnp.logical_not(early))
            def _():
                drain(total, ax_ssem)

    def kernel_matrix(k):
        diag = diag_all[k]
        cross = jnp.concatenate([gather[k, o, 0:4, :] for o in range(CHIPS // 2)], axis=0)
        tri = jnp.concatenate([gather[k, o, 0:4, :] for o in range(CHIPS // 2, CHIPS)], axis=0)
        proj = jnp.concatenate([gather[k, o, 4:6, :] for o in range(CHIPS)], axis=0)
        proj = jnp.concatenate([jnp.where(col_id < rank, proj, 0.0), jnp.where(col_id < rank, 0.0, proj)], axis=0).astype(bf16)
        tri_t, cross_t = tri.T, cross.T
        g_aa = jnp.where(upper, tri, tri_t)
        g_cc = jnp.where(eye, diag, jnp.where(upper, tri_t, tri))
        row_a = jnp.sum(jnp.where(eye, tri, 0.0), axis=0, keepdims=True)
        col_a = jnp.sum(jnp.where(eye, tri, 0.0), axis=1, keepdims=True)
        col_c = jnp.sum(jnp.where(eye, diag, 0.0), axis=1, keepdims=True)
        top = jnp.concatenate([g_aa, cross], axis=1)
        bottom = jnp.concatenate([cross_t, g_cc], axis=1)
        row_all = jnp.concatenate([row_a, diag], axis=1)
        k_top = jnp.exp(-jnp.maximum(col_a + row_all - 2.0 * top, 0.0) * inv_h)
        k_bot = jnp.exp(-jnp.maximum(col_c + row_all - 2.0 * bottom, 0.0) * inv_h)
        kernel = jnp.concatenate([k_top, k_bot], axis=0)
        keep = 1.0 + (scale * two_over_h) * jnp.sum(kernel, axis=1, keepdims=True)
        return kernel.astype(bf16), keep, proj

    def mixed(proj, still, cols):
        return (still - jnp.dot(proj, u_two[:, cols], preferred_element_type=f32)).astype(bf16)

    def moved(kernel_bf, keep, proj, th, still, cols):
        return keep * th + scale * jnp.dot(kernel_bf, mixed(proj, still, cols), preferred_element_type=f32)

    own = slice(0, feat)
    early = functools.reduce(jnp.logical_or, [chip == target for target in EARLY])
    partials(theta[...])
    for copy in swaps:
        copy.wait_send()

    @pl.when(core == 1)
    def _():
        pl.semaphore_wait(barrier, 2 * CHIPS - 1)
        pl.semaphore_signal(go, inc=1, device_id=(ens, partner), device_id_type=MESH)

    @pl.when(core == 0)
    def _():
        pl.semaphore_wait(go, 1)

    @pl.when(core == 0)
    def _():
        pl.delay(LAG)

    scatter()

    @pl.loop(0, NUM_STEPS - 1)
    def _(_):
        base[...] = -((theta[...] - mean_row) * prec_row) - two_over_h * theta[...]
        reduce()
        all_gather(False)
        drain(diag_all.at[0], dg_rsem.at[0])
        drain(gather.at[0], ag_rsem.at[0])
        weights = kernel_matrix(0)
        new = moved(*weights, theta[...], base[...], slice(0, 2 * feat))
        theta[...] = new
        partials(new)
        scatter()
        sent(False)

    def still(th, mean, prec):
        return -((th - mean) * prec) - two_over_h * th

    def back_copy(src, dst):
        return pltpu.make_async_remote_copy(src, dst, back_send, back_recv, device_id=(ens, partner), device_id_type=MESH)

    @pl.when(early)
    def _():
        back = back_copy(theta.at[:, pl.ds(feat, feat)], spare)
        back.start()
        base[:, own] = still(theta[:, own], mean_own[pl.ds(core, 1), :], prec_own[...])
        back.wait()
        base[:, feat:] = still(spare[...], mean_own[pl.ds(other, 1), :], prec_own[...])

    @pl.when(jnp.logical_not(early))
    def _():
        base[...] = still(theta[...], mean_row, prec_row)

    reduce()
    all_gather(True)
    drain(diag_all.at[0], dg_rsem.at[0])
    drain(gather.at[0], ag_rsem.at[0])

    @pl.when(early)
    def _():
        out_ref[core] = moved(*kernel_matrix(0), theta[:, own], base[:, own], own)
        gather[1, chip] = total[...]
        drain(diag_all.at[1], dg_rsem.at[1])
        drain(gather.at[1, others], ag_rsem.at[1])
        out_ref[other] = moved(*kernel_matrix(1), spare[...], base[:, feat:], own)

    @pl.when(jnp.logical_not(early))
    def _():
        weights = kernel_matrix(0)
        kernel_bf, keep, proj = weights
        partners = mixed(proj, base[:, feat:], slice(feat, 2 * feat))
        step = num_part // 4
        for r in range(0, num_part, step):
            rows = slice(r, r + step)
            spare[rows] = keep[rows] * theta[rows, feat:] + scale * jnp.dot(kernel_bf[rows], partners, preferred_element_type=f32)
            back_copy(spare.at[pl.ds(r, step)], out_ref.at[core, pl.ds(r, step)]).start()
        out_ref[core] = moved(*weights, theta[:, own], base[:, own], own)
        back_copy(spare, out_ref.at[other]).wait()

    sent(True)


def solution(mesh):
    feat_count = mesh.shape["feat"]
    data_spec = P("ens", None, "feat")
    mean_spec = P("ens", "feat")
    prec_spec = P(("ens", "feat"))
    factor_spec = P(("ens", "feat"), None)

    def local_steps(particles, target_mean, precision, low_factor):
        _, num_part, feat = particles.shape
        rank = low_factor.shape[1]
        total_feat = feat * feat_count
        bandwidth = 2.0 * total_feat
        consts = (2.0 / bandwidth, 1.0 / bandwidth, 0.25 * total_feat / num_part)
        hbm, vmem = pl.BlockSpec(memory_space=pl.ANY), pl.BlockSpec(memory_space=pltpu.VMEM)
        dma, regular = pltpu.SemaphoreType.DMA, pltpu.SemaphoreType.REGULAR
        f32, bf16 = jnp.float32, jnp.bfloat16
        return pl.pallas_call(
            functools.partial(_kernel, consts),
            name="svgd",
            out_shape=pltpu.VMEM(particles.shape, f32),
            in_specs=[hbm, hbm, hbm, hbm],
            out_specs=vmem,
            scratch_shapes=[
                pltpu.VMEM((num_part, 2 * feat), f32),
                pltpu.VMEM((num_part, 2 * feat), f32),
                pltpu.VMEM((num_part, feat), f32),
                pltpu.VMEM((2, feat), f32),
                pltpu.VMEM((2, feat), f32),
                pltpu.VMEM((1, feat), f32),
                pltpu.VMEM((1, feat), f32),
                pltpu.VMEM((rank, feat), bf16),
                pltpu.VMEM((rank, feat), bf16),
                pltpu.VMEM((CHIPS, 6, HALF), f32),
                pltpu.VMEM((CHIPS, 6, HALF), f32),
                pltpu.VMEM((6, HALF), f32),
                pltpu.VMEM((2, CHIPS, 6, HALF), f32),
                pltpu.VMEM((1, HALF), f32),
                pltpu.VMEM((CHIPS, 1, HALF), f32),
                pltpu.VMEM((1, HALF), f32),
                pltpu.VMEM((2, 1, HALF), f32),
                pltpu.VMEM((2 * rank, 2 * feat), bf16),
                dma((5,)), dma((4,)), dma((4,)), regular, regular, dma, dma, dma, dma((2,)), dma, dma, dma, dma((2,)), dma, dma, dma,
            ],
            compiler_params=pltpu.CompilerParams(collective_id=0, has_side_effects=True),
        )(particles, target_mean, precision.reshape(1, feat), low_factor.T)

    return jax.shard_map(local_steps, mesh=mesh, in_specs=(data_spec, mean_spec, prec_spec, factor_spec), out_specs=data_spec, check_vma=False)
```
